8 devices in a mesh: sp: 2 (over z, y), tp: 4 (over x, core).
Axes of the slice: x: 2, y: 2, z: 1, core: 2. Of those that a mesh axis runs over, the one named last changes fastest.
Arguments:
- tokens: bfloat16 [512, 5120], P('sp')
- context: bfloat16 [512, 5120], replicated
- modulation: float32 [1, 6, 5120], replicated
- w_qkv: bfloat16 [1, 5120, 3, 40, 128], P(None, None, None, 'tp')
- w_out: bfloat16 [1, 40, 128, 5120], P(None, 'tp')
- w_xq: bfloat16 [1, 5120, 40, 128], P(None, None, 'tp')
- w_xkv: bfloat16 [1, 5120, 2, 40, 128], P(None, None, None, 'tp')
- w_xout: bfloat16 [1, 40, 128, 5120], P(None, 'tp')
- w_up: bfloat16 [1, 5120, 20480], P(None, None, 'tp')
- w_down: bfloat16 [1, 20480, 5120], P(None, 'tp')
- w_final: bfloat16 [5120, 64], replicated
Outputs:
- output: float32 [512, 64], P('sp')
All inputs are finite; a program needn't handle non-finite values.
Results may differ from the reference program's by a relative error of at most 0.00672741.
Values are sent between devices in bfloat16 or wider.
A program may use at most 1 GiB of HBM per device.

```python
import math
import jax
import jax.numpy as jnp
from jax import lax

D = 5120
HEADS = 40
FF = 20480
TEXT = 512
DOUT = 64
SEQ = 512
LAYERS = 1

HEAD_DIM = D // HEADS
QBLK = math.gcd(SEQ, 512)
LN_EPS = 1e-6


def setup_inputs(seed: int = 0) -> dict:
    rng_keys = jax.random.split(jax.random.key(seed), 12)
    q_gain = math.sqrt(0.5 * math.log(SEQ))
    x_gain = math.sqrt(0.5 * math.log(TEXT))
    fan_d = D ** -0.5
    centre = jnp.array([0.0, 0.0, 1.5, 0.0, 0.0, 0.5], jnp.float32)[None, :, None]
    spread = jnp.array([0.3, 0.3, 0.4, 0.3, 0.3, 0.2], jnp.float32)[None, :, None]
    qkv_gain = jnp.array([q_gain, 1.0, 1.0], jnp.float32)[None, None, :, None, None]
    tokens = jax.random.normal(rng_keys[0], (SEQ, D), jnp.float32)
    context = jax.random.normal(rng_keys[1], (TEXT, D), jnp.float32)
    modulation = centre + spread * jax.random.normal(rng_keys[2], (LAYERS, 6, D), jnp.float32)
    w_qkv = jax.random.normal(rng_keys[3], (LAYERS, D, 3, HEADS, HEAD_DIM), jnp.float32) * (fan_d * qkv_gain)
    w_out = jax.random.normal(rng_keys[4], (LAYERS, HEADS, HEAD_DIM, D), jnp.float32) * fan_d
    w_xq = jax.random.normal(rng_keys[5], (LAYERS, D, HEADS, HEAD_DIM), jnp.float32) * (fan_d * x_gain)
    w_xkv = jax.random.normal(rng_keys[6], (LAYERS, D, 2, HEADS, HEAD_DIM), jnp.float32) * fan_d
    w_xout = jax.random.normal(rng_keys[7], (LAYERS, HEADS, HEAD_DIM, D), jnp.float32) * fan_d
    w_up = jax.random.normal(rng_keys[8], (LAYERS, D, FF), jnp.float32) * fan_d
    w_down = jax.random.normal(rng_keys[9], (LAYERS, FF, D), jnp.float32) * FF ** -0.5
    w_final = jax.random.normal(rng_keys[10], (D, DOUT), jnp.float32) * fan_d
    return {
        'tokens': tokens.astype(jnp.bfloat16),
        'context': context.astype(jnp.bfloat16),
        'modulation': modulation,
        'w_qkv': w_qkv.astype(jnp.bfloat16),
        'w_out': w_out.astype(jnp.bfloat16),
        'w_xq': w_xq.astype(jnp.bfloat16),
        'w_xkv': w_xkv.astype(jnp.bfloat16),
        'w_xout': w_xout.astype(jnp.bfloat16),
        'w_up': w_up.astype(jnp.bfloat16),
        'w_down': w_down.astype(jnp.bfloat16),
        'w_final': w_final.astype(jnp.bfloat16),
    }


def layer_norm(x_rows):
    row_mean = jnp.mean(x_rows, axis=-1, keepdims=True)
    centred = x_rows - row_mean
    row_var = jnp.mean(centred * centred, axis=-1, keepdims=True)
    return centred * lax.rsqrt(row_var + LN_EPS)


def attend(q_rows, k_rows, v_rows):
    n_blocks = q_rows.shape[0] // QBLK
    q_heads = jnp.transpose(q_rows.astype(jnp.float32), (1, 0, 2)).reshape(HEADS, n_blocks, QBLK, HEAD_DIM)
    k_heads = jnp.transpose(k_rows.astype(jnp.float32), (1, 0, 2))
    v_heads = jnp.transpose(v_rows.astype(jnp.float32), (1, 0, 2))
    score_scale = HEAD_DIM ** -0.5

    def per_head(operands):
        q_blocks, k_one, v_one = operands

        def per_block(q_tile):
            scores = jnp.dot(q_tile, k_one.T, preferred_element_type=jnp.float32) * score_scale
            row_probs = jnp.exp(scores - jnp.max(scores, axis=-1, keepdims=True))
            row_total = jnp.sum(row_probs, axis=-1, keepdims=True)
            mixed_out = jnp.dot(row_probs.astype(jnp.bfloat16).astype(jnp.float32), v_one, preferred_element_type=jnp.float32)
            return (mixed_out / row_total).astype(jnp.bfloat16)

        return lax.map(per_block, q_blocks)

    mixed_all = lax.map(per_head, (q_heads, k_heads, v_heads))
    return jnp.transpose(mixed_all.reshape(HEADS, -1, HEAD_DIM), (1, 0, 2))


def reference(tokens, context, modulation, w_qkv, w_out, w_xq, w_xkv, w_xout, w_up, w_down, w_final):
    def one_block(x_res, layer_w):
        layer_mod, wq_kv, wo_self, wq_cross, wkv_cross, wo_cross, wu_mlp, wd_mlp = layer_w
        h_in = (layer_norm(x_res) * (1.0 + layer_mod[1]) + layer_mod[0]).astype(jnp.bfloat16)
        qkv_rows = jnp.dot(h_in, wq_kv.reshape(D, 3 * D), preferred_element_type=jnp.float32)
        qkv_rows = qkv_rows.astype(jnp.bfloat16).reshape(SEQ, 3, HEADS, HEAD_DIM)
        self_out = attend(qkv_rows[:, 0], qkv_rows[:, 1], qkv_rows[:, 2]).reshape(SEQ, D)
        self_proj = jnp.dot(self_out, wo_self.reshape(D, D), preferred_element_type=jnp.float32).astype(jnp.bfloat16)
        x_res = x_res + layer_mod[2] * self_proj.astype(jnp.float32)
        cross_in = layer_norm(x_res).astype(jnp.bfloat16)
        cross_q = jnp.dot(cross_in, wq_cross.reshape(D, D), preferred_element_type=jnp.float32)
        cross_q = cross_q.astype(jnp.bfloat16).reshape(SEQ, HEADS, HEAD_DIM)
        cross_kv = jnp.dot(context, wkv_cross.reshape(D, 2 * D), preferred_element_type=jnp.float32)
        cross_kv = cross_kv.astype(jnp.bfloat16).reshape(TEXT, 2, HEADS, HEAD_DIM)
        cross_out = attend(cross_q, cross_kv[:, 0], cross_kv[:, 1]).reshape(SEQ, D)
        cross_proj = jnp.dot(cross_out, wo_cross.reshape(D, D), preferred_element_type=jnp.float32).astype(jnp.bfloat16)
        x_res = x_res + cross_proj.astype(jnp.float32)
        mlp_in = (layer_norm(x_res) * (1.0 + layer_mod[4]) + layer_mod[3]).astype(jnp.bfloat16)
        hidden = jax.nn.gelu(jnp.dot(mlp_in, wu_mlp, preferred_element_type=jnp.float32), approximate=True).astype(jnp.bfloat16)
        mlp_out = jnp.dot(hidden, wd_mlp, preferred_element_type=jnp.float32).astype(jnp.bfloat16)
        x_res = x_res + layer_mod[5] * mlp_out.astype(jnp.float32)
        return x_res, None

    stacked = (modulation, w_qkv, w_out, w_xq, w_xkv, w_xout, w_up, w_down)
    x_res = lax.scan(one_block, tokens.astype(jnp.float32), stacked)[0]
    final_in = layer_norm(x_res).astype(jnp.bfloat16)
    return jnp.dot(final_in, w_final, preferred_element_type=jnp.float32)
```

```python
import functools
import jax
import jax.numpy as jnp
from jax import lax
from jax.experimental import pallas as pl
from jax.experimental.pallas import tpu as pltpu
from jax.sharding import PartitionSpec as P

F32 = jnp.float32
BF16 = jnp.bfloat16
LN_EPS = 1e-6
MESH = pl.DeviceIdType.MESH

D = 5120
ROWS = 256
NT = 20
KC = 4
HL = 10
NH = 2
RH = ROWS // NH
CB = RH // 2
OB = RH // 4
NSLOT = 40
HALVES = tuple(range(NH))


def dot(a, b):
    return jnp.dot(a, b, preferred_element_type=F32)


def dot_nt(a, b):
    return lax.dot_general(a, b, (((1,), (1,)), ((), ())), preferred_element_type=F32)


def block_kernel(q_hbm, kv_hbm, kvo_hbm, xkv_hbm, tok_hbm, mod_ref, w_out, w_xq, w_xout, w_up, w_down, wf_hbm,
                 out_ref,
                 ring, part, dsum, xin, xres, hbuf, ubuf, qacc, obuf, qbuf, kvs, kvx, tok, wf, obout,
                 rsem, lsem, ds_s, ds_r, xs_s, xs_r, ax_s, ax_r, ad_s, ad_r, af_s, af_r, os_s, os_r):
    sp = lax.axis_index('sp')
    tp = lax.axis_index('tp')
    x = tp // 2
    c = tp % 2
    partner = (sp, 2 * x + (1 - c))
    across = (sp, 2 * (1 - x) + c)
    diagonal = (sp, 2 * (1 - x) + (1 - c))

    def kslice(kc):
        return pl.ds(kc * 1280, 1280)

    def nslice(nb):
        return pl.ds(nb * 256, 256)

    def start_cols(w, kc, nb, slot):
        pltpu.make_async_copy(w.at[kslice(kc), nslice(nb)], ring.at[slot], rsem.at[slot]).start()

    def start_xq(kc, b, slot):
        for hh in range(2):
            pltpu.make_async_copy(w_xq.at[2 * b + hh, kslice(kc), :], ring.at[slot, :, pl.ds(128 * hh, 128)],
                                  rsem.at[slot]).start()

    def wait_block(slot):
        pltpu.make_async_copy(w_out.at[pl.ds(0, 1280), pl.ds(0, 256)], ring.at[slot], rsem.at[slot]).wait()

    def start_down(g, i, slot):
        start_cols(w_down, i % 4, 5 * g + i // 4, slot)

    own_rows = [a * RH + c * CB + x * OB for a in HALVES]
    loads = [
        (q_hbm, qbuf, 0),
        (kv_hbm, kvs.at[:, :, pl.ds(0, 256), :], 1),
        (kvo_hbm, kvs.at[:, :, pl.ds(256, 256), :], 2),
        (xkv_hbm, kvx, 3),
        (wf_hbm, wf, 4),
    ] + [(tok_hbm.at[pl.ds(pl.multiple_of(own_rows[a], OB), OB), :], tok.at[a], 5 + a) for a in HALVES]

    def load(i):
        s, d, k = loads[i]
        return pltpu.make_async_copy(s, d, lsem.at[k])

    for i in range(3):
        load(i).start()

    @pl.loop(0, NT)
    def _(t):
        start_cols(w_out, 0, t, t)

    for i in range(3, len(loads)):
        load(i).start()

    @pl.loop(0, NT)
    def _(i):
        start_xq(i // 5, i % 5, 20 + i)

    barrier = pltpu.get_barrier_semaphore()
    for peer in (partner, across, diagonal):
        pl.semaphore_signal(barrier, inc=1, device_id=peer, device_id_type=MESH)

    scale = 128 ** -0.5

    def attend(qh, kv, h):
        s1 = dot_nt(qh, kv[0, h, 0:256, :]) * scale
        s2 = dot_nt(qh, kv[0, h, 256:512, :]) * scale
        m = jnp.maximum(jnp.max(s1, axis=-1, keepdims=True), jnp.max(s2, axis=-1, keepdims=True))
        p1 = jnp.exp(s1 - m)
        p2 = jnp.exp(s2 - m)
        total = jnp.sum(p1, axis=-1, keepdims=True) + jnp.sum(p2, axis=-1, keepdims=True)
        o = dot(p1.astype(BF16), kv[1, h, 0:256, :]) + dot(p2.astype(BF16), kv[1, h, 256:512, :])
        return (o / total).astype(BF16)

    def d2d(a, t):
        src = part.at[t, pl.ds(pl.multiple_of(a * RH + (1 - c) * CB, OB), CB), :]
        return pltpu.make_async_remote_copy(src_ref=src, dst_ref=dsum.at[a, t], send_sem=ds_s.at[a, t],
                                            recv_sem=ds_r.at[a, t], device_id=partner, device_id_type=MESH)

    def xsend(a, t):
        src = dsum.at[a, t, pl.ds(pl.multiple_of((1 - x) * OB, OB), OB), :]
        return pltpu.make_async_remote_copy(src_ref=src, dst_ref=xin.at[a, t], send_sem=xs_s.at[a, t],
                                            recv_sem=xs_r.at[a, t], device_id=across, device_id_type=MESH)

    def core_sum(a, t):
        d2d(a, t).wait_recv()
        dsum[a, t] = dsum[a, t] + part[t, pl.ds(pl.multiple_of(a * RH + c * CB, OB), CB), :]

    def rs_loop(compute, compute_halves, send_halves, per_iter, lag):
        iters = NT // per_iter

        @pl.loop(0, iters + lag)
        def _(i):
            @pl.when(i < iters)
            def _():
                for u in range(per_iter):
                    compute(i * per_iter + u)

            @pl.when(i >= lag)
            def _():
                for u in range(per_iter):
                    for a in send_halves:
                        core_sum(a, (i - lag) * per_iter + u)

            @pl.when(i < iters)
            def _():
                for u in range(per_iter):
                    for a in compute_halves:
                        d2d(a, i * per_iter + u).start()

            @pl.when(i >= lag)
            def _():
                for u in range(per_iter):
                    for a in send_halves:
                        xsend(a, (i - lag) * per_iter + u).start()

    def hrows(core, chip, a):
        return pl.ds(pl.multiple_of(a * RH + core * CB + chip * OB, OB), OB)

    def gather_copy(kc, rows, ssem, rsem_, peer):
        ref = hbuf.at[pl.ds(kc * 5, 5), rows, :]
        return pltpu.make_async_remote_copy(src_ref=ref, dst_ref=ref, send_sem=ssem, recv_sem=rsem_,
                                            device_id=peer, device_id_type=MESH)

    def g_across(a, kc, chip):
        return gather_copy(kc, hrows(c, chip, a), ax_s.at[a, kc], ax_r.at[a, kc], across)

    def g_partner(a, kc, core):
        return gather_copy(kc, hrows(core, x, a), ad_s.at[a, kc], ad_r.at[a, kc], partner)

    def g_forward(a, kc, core):
        return gather_copy(kc, hrows(core, 1 - x, a), af_s.at[a, kc], af_r.at[a, kc], partner)

    def modrow(r, t):
        return mod_ref[r, 0:1, pl.ds(pl.multiple_of(t * 256, 256), 256)]

    def residual(a, gate, first):
        def body(i, acc):
            for u in range(4):
                t = i * 4 + u
                xsend(a, t).wait()
                d2d(a, t).wait_send()
                proj = (dsum[a, t, pl.ds(pl.multiple_of(x * OB, OB), OB), :] + xin[a, t]).astype(BF16).astype(F32)
                if gate is not None:
                    proj = modrow(gate, t) * proj
                if first:
                    prev = tok[a, :, pl.ds(pl.multiple_of(t * 256, 256), 256)].astype(F32)
                else:
                    prev = xres[a, t]
                new = prev + proj
                xres[a, t] = new
                acc = acc + new
            return acc
        acc = lax.fori_loop(0, NT // 4, body, jnp.zeros((OB, 256), F32))
        return jnp.sum(acc, axis=-1, keepdims=True)

    def stats(a, row_sum):
        mean = row_sum / D

        def body(i, acc):
            for u in range(4):
                d_ = xres[a, i * 4 + u] - mean
                acc = acc + d_ * d_
            return acc
        acc = lax.fori_loop(0, NT // 4, body, jnp.zeros((OB, 256), F32))
        var = jnp.sum(acc, axis=-1, keepdims=True) / D
        return mean, lax.rsqrt(var + LN_EPS)

    def norm_and_send(a, gate, first, shift, gain):
        mean, inv = stats(a, residual(a, gate, first))

        @pl.loop(0, KC)
        def _(kc):
            for u in range(5):
                t = kc * 5 + u
                h = (xres[a, t] - mean) * inv
                if gain is not None:
                    h = h * (1.0 + modrow(gain, t)) + modrow(shift, t)
                hbuf[t, hrows(c, x, a), :] = h.astype(BF16)
            g_across(a, kc, x).start()
            g_partner(a, kc, c).start()

    def gather_forward(a, kc):
        g_across(a, kc, 1 - x).wait_recv()
        g_forward(a, kc, c).start()

    def gather_wait(a, kc):
        g_partner(a, kc, 1 - c).wait_recv()
        g_forward(a, kc, 1 - c).wait_recv()
        g_across(a, kc, x).wait_send()
        g_partner(a, kc, c).wait_send()
        g_forward(a, kc, c).wait_send()

    def mm(lhs, slot):
        acc = dot(lhs(0), ring[slot, 0:256, :])
        for j in range(1, 5):
            acc = acc + dot(lhs(j), ring[slot, 256 * j:256 * (j + 1), :])
        return acc

    for i in range(3):
        load(i).wait()

    @pl.loop(0, HL // 2)
    def _(b):
        for hh in range(2):
            for a in HALVES:
                rows = pl.ds(a * RH, RH)
                obuf[b, rows, 128 * hh:128 * (hh + 1)] = attend(qbuf[2 * b + hh, rows, :], kvs, 2 * b + hh)

    pl.semaphore_wait(barrier, 3)

    def out_tile(t):
        wait_block(t)
        part[t] = mm(lambda j: obuf[j], t)
        start_cols(w_xout, 0, t, t)

    rs_loop(out_tile, HALVES, HALVES[:1], 4, 2)
    for a in HALVES[1:]:
        @pl.loop(0, NT)
        def _(t):
            core_sum(a, t)
            xsend(a, t).start()

    for i in range(3, len(loads)):
        load(i).wait()
    for a in HALVES:
        norm_and_send(a, 2, True, None, None)

    for a in HALVES:
        rows = pl.ds(a * RH, RH)
        last = a == HALVES[-1]
        for b in range(5):
            qacc[b, rows, :] = jnp.zeros((RH, 256), F32)

        gather_forward(a, 0)

        @pl.loop(0, KC)
        def _(kc):
            @pl.when(kc < KC - 1)
            def _():
                gather_forward(a, kc + 1)
            gather_wait(a, kc)
            for b in range(5):
                slot = 20 + kc * 5 + b
                if a == 0:
                    wait_block(slot)
                qacc[b, rows, :] += mm(lambda j: hbuf[kc * 5 + j, rows, :], slot)
                if last:
                    start_cols(w_up, 0, kc * 5 + b, slot)

        @pl.loop(0, HL // 2)
        def _(b):
            for hh in range(2):
                qh = qacc[b, rows, 128 * hh:128 * (hh + 1)].astype(BF16)
                obuf[b, rows, 128 * hh:128 * (hh + 1)] = attend(qh, kvx, 2 * b + hh)

        def xout_tile(t):
            if a == 0:
                wait_block(t)
            part[t, rows, :] = mm(lambda j: obuf[j, rows, :], t)
            if last:
                start_cols(w_up, 1, t, t)

        rs_loop(xout_tile, (a,), (a,), 4, 2)

    for a in HALVES:
        norm_and_send(a, None, False, 3, 4)

    for a in HALVES[:-1]:
        @pl.loop(0, KC)
        def _(kc):
            gather_forward(a, kc)
    gather_forward(HALVES[-1], 0)
    for kc in range(KC):
        if kc < KC - 1:
            gather_forward(HALVES[-1], kc + 1)
        for a in HALVES:
            gather_wait(a, kc)
        base = 20 if kc % 2 == 0 else 0

        @pl.loop(0, NT // 4)
        def _(i):
            for u in range(4):
                nb = i * 4 + u
                wait_block(base + nb)
                acc = mm(lambda j: hbuf[kc * 5 + j], base + nb)
                if kc > 0:
                    acc = part[nb] + acc
                if kc < KC - 1:
                    part[nb] = acc
                else:
                    ubuf[nb] = jax.nn.gelu(acc, approximate=True).astype(BF16)
                if kc < 2:
                    start_cols(w_up, kc + 2, nb, base + nb)
                else:
                    start_down(kc - 2, nb, base + nb)

    def down_tile(t):
        g = t // 5
        base = 20 * ((g + 1) % 2) + 4 * (t % 5)
        acc = None
        for kc in range(KC):
            wait_block(base + kc)
            new = mm(lambda j: ubuf[5 * kc + j], base + kc)
            acc = new if acc is None else acc + new
        part[t] = acc

        @pl.when(g < 2)
        def _():
            for kc in range(KC):
                start_cols(w_down, kc, t + 10, base + kc)

    rs_loop(down_tile, HALVES, HALVES, 1, 2)

    def out_copy(a, peer, k, core, chip):
        ref = obout.at[hrows(core, chip, a), :]
        return pltpu.make_async_remote_copy(src_ref=ref, dst_ref=ref, send_sem=os_s.at[a, k], recv_sem=os_r.at[a, k],
                                            device_id=peer, device_id_type=MESH)

    for a in HALVES:
        mean, inv = stats(a, residual(a, 5, False))

        def body(i, acc):
            for u in range(4):
                t = i * 4 + u
                fin = ((xres[a, t] - mean) * inv).astype(BF16)
                acc = acc + dot_nt(fin, wf[:, pl.ds(pl.multiple_of(t * 256, 256), 256)])
            return acc
        acc = lax.fori_loop(0, NT // 4, body, jnp.zeros((OB, 64), F32))
        obout[hrows(c, x, a), :] = jnp.concatenate([acc, jnp.zeros((OB, 64), F32)], axis=1)
        out_copy(a, across, 0, c, x).start()
        out_copy(a, partner, 1, c, x).start()
        out_copy(a, diagonal, 2, c, x).start()
    for a in HALVES:
        out_copy(a, across, 0, c, 1 - x).wait()
        out_copy(a, partner, 1, 1 - c, x).wait()
        out_copy(a, diagonal, 2, 1 - c, 1 - x).wait()
    out_ref[...] = obout[:, 0:64]


def block_call(args):
    any_spec = pl.BlockSpec(memory_space=pl.ANY)
    vmem_spec = pl.BlockSpec(memory_space=pltpu.VMEM)
    sem = pltpu.SemaphoreType.DMA
    return pl.pallas_call(
        block_kernel,
        out_shape=jax.ShapeDtypeStruct((ROWS, 64), F32),
        in_specs=[any_spec] * 5 + [vmem_spec] + [any_spec] * 6,
        out_specs=vmem_spec,
        scratch_shapes=[
            pltpu.VMEM((NSLOT, 1280, 256), BF16),
            pltpu.VMEM((NT, ROWS, 256), F32),
            pltpu.VMEM((NH, NT, CB, 256), F32),
            pltpu.VMEM((NH, NT, OB, 256), F32),
            pltpu.VMEM((NH, NT, OB, 256), F32),
            pltpu.VMEM((NT, ROWS, 256), BF16),
            pltpu.VMEM((NT, ROWS, 256), BF16),
            pltpu.VMEM((5, ROWS, 256), F32),
            pltpu.VMEM((5, ROWS, 256), BF16),
            pltpu.VMEM((HL, ROWS, 128), BF16),
            pltpu.VMEM((2, HL, 512, 128), BF16),
            pltpu.VMEM((2, HL, 512, 128), BF16),
            pltpu.VMEM((NH, OB, D), BF16),
            pltpu.VMEM((64, D), BF16),
            pltpu.VMEM((ROWS, 128), F32),
            sem((NSLOT,)), sem((8,)),
            sem((NH, NT)), sem((NH, NT)), sem((NH, NT)), sem((NH, NT)),
            sem((NH, KC)), sem((NH, KC)), sem((NH, KC)), sem((NH, KC)), sem((NH, KC)), sem((NH, KC)),
            sem((NH, 3)), sem((NH, 3)),
        ],
        compiler_params=pltpu.CompilerParams(collective_id=0, has_side_effects=True, vmem_limit_bytes=63 * 2**20),
        cost_estimate=pl.CostEstimate(flops=2 * 256 * 72 * 10**6, bytes_accessed=150 * 10**6, transcendentals=4 * 10**6),
        name='dit_block',
    )(*args)


def layer_norm(x_rows):
    row_mean = jnp.mean(x_rows, axis=-1, keepdims=True)
    centred = x_rows - row_mean
    row_var = jnp.mean(centred * centred, axis=-1, keepdims=True)
    return centred * lax.rsqrt(row_var + LN_EPS)


def solution(mesh):
    def device_step(tokens, context, modulation, w_qkv, w_out, w_xq, w_xkv, w_xout, w_up, w_down, w_final):
        mod = modulation[0]
        h_in = (layer_norm(tokens.astype(F32)) * (1.0 + mod[1]) + mod[0]).astype(BF16)
        kv = jnp.einsum('sd,dchk->schk', h_in, w_qkv[0][:, 1:3], preferred_element_type=F32).astype(BF16)
        kv = jnp.transpose(kv, (1, 2, 0, 3))
        kv_other = lax.ppermute(kv, 'sp', [(0, 1), (1, 0)])
        q = jnp.einsum('sd,dhk->shk', h_in, w_qkv[0][:, 0], preferred_element_type=F32).astype(BF16)
        q = jnp.transpose(q, (1, 0, 2))
        xkv = jnp.einsum('td,dchk->tchk', context, w_xkv[0], preferred_element_type=F32).astype(BF16)
        xkv = jnp.transpose(xkv, (1, 2, 0, 3))
        return block_call((
            q, kv, kv_other, xkv, tokens, jnp.transpose(modulation, (1, 0, 2)),
            w_out[0].reshape(1280, D), jnp.transpose(w_xq[0], (1, 0, 2)), w_xout[0].reshape(1280, D),
            w_up[0], w_down[0], jnp.transpose(w_final)))

    in_specs = (P('sp', None), P(), P(), P(None, None, None, 'tp', None), P(None, 'tp', None, None),
                P(None, None, 'tp', None), P(None, None, None, 'tp', None), P(None, 'tp', None, None),
                P(None, None, 'tp'), P(None, 'tp', None), P())
    return jax.shard_map(device_step, mesh=mesh, in_specs=in_specs, out_specs=P('sp', None), check_vma=False)
```

```python
import functools
import jax
import jax.numpy as jnp
from jax import lax
from jax.experimental import pallas as pl
from jax.experimental.pallas import tpu as pltpu
from jax.sharding import PartitionSpec as P

F32 = jnp.float32
BF16 = jnp.bfloat16
LN_EPS = 1e-6
MESH = pl.DeviceIdType.MESH

D = 5120
ROWS = 256
NT = 20
KC = 4
HL = 10
NH = 2
RH = ROWS // NH
CB = RH // 2
OB = RH // 4
NSLOT = 40
HALVES = tuple(range(NH))
GA = 4
GD = 2


def dot(a, b):
    return jnp.dot(a, b, preferred_element_type=F32)


def dot_nt(a, b):
    return lax.dot_general(a, b, (((1,), (1,)), ((), ())), preferred_element_type=F32)


def block_kernel(q_hbm, kv_hbm, kvo_hbm, xkv_hbm, tok_hbm, mod_ref, w_out, w_xq, w_xout, w_up, w_down, wf_hbm,
                 out_ref,
                 ring, part, dsum, xin, xres, hbuf, ubuf, qacc, obuf, qbuf, kvs, kvx, tok, wf, obout,
                 rsem, lsem, ds_s, ds_r, xs_s, xs_r, ax_s, ax_r, ad_s, ad_r, af_s, af_r, os_s, os_r):
    sp = lax.axis_index('sp')
    tp = lax.axis_index('tp')
    x = tp // 2
    c = tp % 2
    partner = (sp, 2 * x + (1 - c))
    across = (sp, 2 * (1 - x) + c)
    diagonal = (sp, 2 * (1 - x) + (1 - c))

    def kslice(kc):
        return pl.ds(kc * 1280, 1280)

    def nslice(nb):
        return pl.ds(nb * 256, 256)

    def start_cols(w, kc, nb, slot):
        pltpu.make_async_copy(w.at[kslice(kc), nslice(nb)], ring.at[slot], rsem.at[slot]).start()

    def start_xq(kc, b, slot):
        for hh in range(2):
            pltpu.make_async_copy(w_xq.at[2 * b + hh, kslice(kc), :], ring.at[slot, :, pl.ds(128 * hh, 128)],
                                  rsem.at[slot]).start()

    def wait_block(slot):
        pltpu.make_async_copy(w_out.at[pl.ds(0, 1280), pl.ds(0, 256)], ring.at[slot], rsem.at[slot]).wait()

    def start_down(g, i, slot):
        start_cols(w_down, i % 4, 5 * g + i // 4, slot)

    own_rows = [a * RH + c * CB + x * OB for a in HALVES]
    loads = [
        (q_hbm, qbuf, 0),
        (kv_hbm, kvs.at[:, :, pl.ds(0, 256), :], 1),
        (kvo_hbm, kvs.at[:, :, pl.ds(256, 256), :], 2),
        (xkv_hbm, kvx, 3),
        (wf_hbm, wf, 4),
    ] + [(tok_hbm.at[pl.ds(pl.multiple_of(own_rows[a], OB), OB), :], tok.at[a], 5 + a) for a in HALVES]

    def load(i):
        s, d, k = loads[i]
        return pltpu.make_async_copy(s, d, lsem.at[k])

    for i in range(3):
        load(i).start()

    @pl.loop(0, NT)
    def _(t):
        start_cols(w_out, 0, t, t)

    for i in range(3, len(loads)):
        load(i).start()

    @pl.loop(0, NT)
    def _(i):
        start_xq(i // 5, i % 5, 20 + i)

    barrier = pltpu.get_barrier_semaphore()
    for peer in (partner, across, diagonal):
        pl.semaphore_signal(barrier, inc=1, device_id=peer, device_id_type=MESH)

    scale = 128 ** -0.5

    def attend(qh, kv, h):
        s1 = dot_nt(qh, kv[0, h, 0:256, :]) * scale
        s2 = dot_nt(qh, kv[0, h, 256:512, :]) * scale
        m = jnp.maximum(jnp.max(s1, axis=-1, keepdims=True), jnp.max(s2, axis=-1, keepdims=True))
        p1 = jnp.exp(s1 - m)
        p2 = jnp.exp(s2 - m)
        total = jnp.sum(p1, axis=-1, keepdims=True) + jnp.sum(p2, axis=-1, keepdims=True)
        o = dot(p1.astype(BF16), kv[1, h, 0:256, :]) + dot(p2.astype(BF16), kv[1, h, 256:512, :])
        return (o / total).astype(BF16)

    def d2d(a, i, g):
        src = part.at[pl.ds(i * g, g), pl.ds(pl.multiple_of(a * RH + (1 - c) * CB, OB), CB), :]
        return pltpu.make_async_remote_copy(src_ref=src, dst_ref=dsum.at[a, pl.ds(i * g, g)], send_sem=ds_s.at[a, i],
                                            recv_sem=ds_r.at[a, i], device_id=partner, device_id_type=MESH)

    def xsend(a, i, g):
        src = dsum.at[a, pl.ds(i * g, g), pl.ds(pl.multiple_of((1 - x) * OB, OB), OB), :]
        return pltpu.make_async_remote_copy(src_ref=src, dst_ref=xin.at[a, pl.ds(i * g, g)], send_sem=xs_s.at[a, i],
                                            recv_sem=xs_r.at[a, i], device_id=across, device_id_type=MESH)

    def core_sum(a, i, g):
        d2d(a, i, g).wait_recv()
        for u in range(g):
            t = i * g + u
            dsum[a, t] = dsum[a, t] + part[t, pl.ds(pl.multiple_of(a * RH + c * CB, OB), CB), :]

    def rs_loop(compute, compute_halves, send_halves, g, lag):
        iters = NT // g

        @pl.loop(0, iters + lag)
        def _(i):
            @pl.when(i < iters)
            def _():
                compute(i)

            @pl.when(i >= lag)
            def _():
                for a in send_halves:
                    core_sum(a, i - lag, g)

            @pl.when(i < iters)
            def _():
                for a in compute_halves:
                    d2d(a, i, g).start()

            @pl.when(i >= lag)
            def _():
                for a in send_halves:
                    xsend(a, i - lag, g).start()

    def hrows(core, chip, a):
        return pl.ds(pl.multiple_of(a * RH + core * CB + chip * OB, OB), OB)

    def gather_copy(kc, rows, ssem, rsem_, peer):
        ref = hbuf.at[pl.ds(kc * 5, 5), rows, :]
        return pltpu.make_async_remote_copy(src_ref=ref, dst_ref=ref, send_sem=ssem, recv_sem=rsem_,
                                            device_id=peer, device_id_type=MESH)

    def g_across(a, kc, chip):
        return gather_copy(kc, hrows(c, chip, a), ax_s.at[a, kc], ax_r.at[a, kc], across)

    def g_partner(a, kc, core):
        return gather_copy(kc, hrows(core, x, a), ad_s.at[a, kc], ad_r.at[a, kc], partner)

    def g_forward(a, kc, core):
        return gather_copy(kc, hrows(core, 1 - x, a), af_s.at[a, kc], af_r.at[a, kc], partner)

    def modrow(r, t):
        return mod_ref[r, 0:1, pl.ds(pl.multiple_of(t * 256, 256), 256)]

    def residual(a, gate, first, g):
        def body(i, acc):
            xsend(a, i, g).wait()
            d2d(a, i, g).wait_send()
            for u in range(g):
                t = i * g + u
                proj = (dsum[a, t, pl.ds(pl.multiple_of(x * OB, OB), OB), :] + xin[a, t]).astype(BF16).astype(F32)
                if gate is not None:
                    proj = modrow(gate, t) * proj
                if first:
                    prev = tok[a, :, pl.ds(pl.multiple_of(t * 256, 256), 256)].astype(F32)
                else:
                    prev = xres[a, t]
                new = prev + proj
                xres[a, t] = new
                acc = acc + new
            return acc
        acc = lax.fori_loop(0, NT // g, body, jnp.zeros((OB, 256), F32))
        return jnp.sum(acc, axis=-1, keepdims=True)

    def stats(a, row_sum):
        mean = row_sum / D

        def body(i, acc):
            for u in range(4):
                d_ = xres[a, i * 4 + u] - mean
                acc = acc + d_ * d_
            return acc
        acc = lax.fori_loop(0, NT // 4, body, jnp.zeros((OB, 256), F32))
        var = jnp.sum(acc, axis=-1, keepdims=True) / D
        return mean, lax.rsqrt(var + LN_EPS)

    def norm_and_send(a, gate, first, shift, gain):
        mean, inv = stats(a, residual(a, gate, first, GA))

        @pl.loop(0, KC)
        def _(kc):
            for u in range(5):
                t = kc * 5 + u
                h = (xres[a, t] - mean) * inv
                if gain is not None:
                    h = h * (1.0 + modrow(gain, t)) + modrow(shift, t)
                hbuf[t, hrows(c, x, a), :] = h.astype(BF16)
            g_across(a, kc, x).start()
            g_partner(a, kc, c).start()

    def gather_forward(a, kc):
        g_across(a, kc, 1 - x).wait_recv()
        g_forward(a, kc, c).start()

    def gather_wait(a, kc):
        g_partner(a, kc, 1 - c).wait_recv()
        g_forward(a, kc, 1 - c).wait_recv()
        g_across(a, kc, x).wait_send()
        g_partner(a, kc, c).wait_send()
        g_forward(a, kc, c).wait_send()

    def mm(lhs, slot):
        acc = dot(lhs(0), ring[slot, 0:256, :])
        for j in range(1, 5):
            acc = acc + dot(lhs(j), ring[slot, 256 * j:256 * (j + 1), :])
        return acc

    for i in range(3):
        load(i).wait()

    @pl.loop(0, HL // 2)
    def _(b):
        for hh in range(2):
            for a in HALVES:
                rows = pl.ds(a * RH, RH)
                obuf[b, rows, 128 * hh:128 * (hh + 1)] = attend(qbuf[2 * b + hh, rows, :], kvs, 2 * b + hh)

    pl.semaphore_wait(barrier, 3)

    def out_tiles(i):
        for u in range(GA):
            wait_block(i * GA + u)
        for u in range(GA):
            part[i * GA + u] = mm(lambda j: obuf[j], i * GA + u)
        for u in range(GA):
            start_cols(w_xout, 0, i * GA + u, i * GA + u)

    rs_loop(out_tiles, HALVES, HALVES[:1], GA, 2)
    for a in HALVES[1:]:
        @pl.loop(0, NT // GA)
        def _(i):
            core_sum(a, i, GA)
            xsend(a, i, GA).start()

    for i in range(3, len(loads)):
        load(i).wait()
    for a in HALVES:
        norm_and_send(a, 2, True, None, None)

    for a in HALVES:
        rows = pl.ds(a * RH, RH)
        last = a == HALVES[-1]
        for b in range(5):
            qacc[b, rows, :] = jnp.zeros((RH, 256), F32)

        gather_forward(a, 0)

        @pl.loop(0, KC)
        def _(kc):
            @pl.when(kc < KC - 1)
            def _():
                gather_forward(a, kc + 1)
            gather_wait(a, kc)
            if a == 0:
                for b in range(5):
                    wait_block(20 + kc * 5 + b)
            for b in range(5):
                qacc[b, rows, :] += mm(lambda j: hbuf[kc * 5 + j, rows, :], 20 + kc * 5 + b)
            if last:
                for b in range(5):
                    start_cols(w_up, 0, kc * 5 + b, 20 + kc * 5 + b)

        @pl.loop(0, HL // 2)
        def _(b):
            for hh in range(2):
                qh = qacc[b, rows, 128 * hh:128 * (hh + 1)].astype(BF16)
                obuf[b, rows, 128 * hh:128 * (hh + 1)] = attend(qh, kvx, 2 * b + hh)

        def xout_tiles(i):
            if a == 0:
                for u in range(GA):
                    wait_block(i * GA + u)
            for u in range(GA):
                part[i * GA + u, rows, :] = mm(lambda j: obuf[j, rows, :], i * GA + u)
            if last:
                for u in range(GA):
                    start_cols(w_up, 1, i * GA + u, i * GA + u)

        rs_loop(xout_tiles, (a,), (a,), GA, 2)

    for a in HALVES:
        norm_and_send(a, None, False, 3, 4)

    for a in HALVES[:-1]:
        @pl.loop(0, KC)
        def _(kc):
            gather_forward(a, kc)
    gather_forward(HALVES[-1], 0)
    for kc in range(KC):
        if kc < KC - 1:
            gather_forward(HALVES[-1], kc + 1)
        for a in HALVES:
            gather_wait(a, kc)
        base = 20 if kc % 2 == 0 else 0

        @pl.loop(0, NT // 4)
        def _(i):
            for u in range(4):
                wait_block(base + i * 4 + u)
            for u in range(4):
                nb = i * 4 + u
                acc = mm(lambda j: hbuf[kc * 5 + j], base + nb)
                if kc > 0:
                    acc = part[nb] + acc
                if kc < KC - 1:
                    part[nb] = acc
                else:
                    ubuf[nb] = jax.nn.gelu(acc, approximate=True).astype(BF16)
            for u in range(4):
                nb = i * 4 + u
                if kc < 2:
                    start_cols(w_up, kc + 2, nb, base + nb)
                else:
                    start_down(kc - 2, nb, base + nb)

    def down_tiles(i):
        def slot(t, kc):
            return 20 * ((t // 5 + 1) % 2) + 4 * (t % 5) + kc

        for u in range(GD):
            for kc in range(KC):
                wait_block(slot(i * GD + u, kc))
        for u in range(GD):
            t = i * GD + u
            acc = mm(lambda j: ubuf[j], slot(t, 0))
            for kc in range(1, KC):
                acc = acc + mm(lambda j: ubuf[5 * kc + j], slot(t, kc))
            part[t] = acc
        for u in range(GD):
            t = i * GD + u

            @pl.when(t < 10)
            def _():
                for kc in range(KC):
                    start_cols(w_down, kc, t + 10, slot(t, kc))

    rs_loop(down_tiles, HALVES, HALVES, GD, 1)

    def out_copy(a, peer, k, core, chip):
        ref = obout.at[hrows(core, chip, a), :]
        return pltpu.make_async_remote_copy(src_ref=ref, dst_ref=ref, send_sem=os_s.at[a, k], recv_sem=os_r.at[a, k],
                                            device_id=peer, device_id_type=MESH)

    for a in HALVES:
        mean, inv = stats(a, residual(a, 5, False, GD))

        def body(i, acc):
            for u in range(4):
                t = i * 4 + u
                fin = ((xres[a, t] - mean) * inv).astype(BF16)
                acc = acc + dot_nt(fin, wf[:, pl.ds(pl.multiple_of(t * 256, 256), 256)])
            return acc
        acc = lax.fori_loop(0, NT // 4, body, jnp.zeros((OB, 64), F32))
        obout[hrows(c, x, a), :] = jnp.concatenate([acc, jnp.zeros((OB, 64), F32)], axis=1)
        out_copy(a, across, 0, c, x).start()
        out_copy(a, partner, 1, c, x).start()
        out_copy(a, diagonal, 2, c, x).start()
    for a in HALVES:
        out_copy(a, across, 0, c, 1 - x).wait()
        out_copy(a, partner, 1, 1 - c, x).wait()
        out_copy(a, diagonal, 2, 1 - c, 1 - x).wait()
    out_ref[...] = obout[:, 0:64]


def block_call(args):
    any_spec = pl.BlockSpec(memory_space=pl.ANY)
    vmem_spec = pl.BlockSpec(memory_space=pltpu.VMEM)
    sem = pltpu.SemaphoreType.DMA
    return pl.pallas_call(
        block_kernel,
        out_shape=jax.ShapeDtypeStruct((ROWS, 64), F32),
        in_specs=[any_spec] * 5 + [vmem_spec] + [any_spec] * 6,
        out_specs=vmem_spec,
        scratch_shapes=[
            pltpu.VMEM((NSLOT, 1280, 256), BF16),
            pltpu.VMEM((NT, ROWS, 256), F32),
            pltpu.VMEM((NH, NT, CB, 256), F32),
            pltpu.VMEM((NH, NT, OB, 256), F32),
            pltpu.VMEM((NH, NT, OB, 256), F32),
            pltpu.VMEM((NT, ROWS, 256), BF16),
            pltpu.VMEM((NT, ROWS, 256), BF16),
            pltpu.VMEM((5, ROWS, 256), F32),
            pltpu.VMEM((5, ROWS, 256), BF16),
            pltpu.VMEM((HL, ROWS, 128), BF16),
            pltpu.VMEM((2, HL, 512, 128), BF16),
            pltpu.VMEM((2, HL, 512, 128), BF16),
            pltpu.VMEM((NH, OB, D), BF16),
            pltpu.VMEM((64, D), BF16),
            pltpu.VMEM((ROWS, 128), F32),
            sem((NSLOT,)), sem((8,)),
            sem((NH, NT)), sem((NH, NT)), sem((NH, NT)), sem((NH, NT)),
            sem((NH, KC)), sem((NH, KC)), sem((NH, KC)), sem((NH, KC)), sem((NH, KC)), sem((NH, KC)),
            sem((NH, 3)), sem((NH, 3)),
        ],
        compiler_params=pltpu.CompilerParams(collective_id=0, has_side_effects=True, vmem_limit_bytes=63 * 2**20),
        cost_estimate=pl.CostEstimate(flops=2 * 256 * 72 * 10**6, bytes_accessed=150 * 10**6, transcendentals=4 * 10**6),
        name='dit_block',
    )(*args)


def layer_norm(x_rows):
    row_mean = jnp.mean(x_rows, axis=-1, keepdims=True)
    centred = x_rows - row_mean
    row_var = jnp.mean(centred * centred, axis=-1, keepdims=True)
    return centred * lax.rsqrt(row_var + LN_EPS)


def solution(mesh):
    def device_step(tokens, context, modulation, w_qkv, w_out, w_xq, w_xkv, w_xout, w_up, w_down, w_final):
        mod = modulation[0]
        h_in = (layer_norm(tokens.astype(F32)) * (1.0 + mod[1]) + mod[0]).astype(BF16)
        kv = jnp.einsum('sd,dchk->schk', h_in, w_qkv[0][:, 1:3], preferred_element_type=F32).astype(BF16)
        kv = jnp.transpose(kv, (1, 2, 0, 3))
        kv_other = lax.ppermute(kv, 'sp', [(0, 1), (1, 0)])
        q = jnp.einsum('sd,dhk->shk', h_in, w_qkv[0][:, 0], preferred_element_type=F32).astype(BF16)
        q = jnp.transpose(q, (1, 0, 2))
        xkv = jnp.einsum('td,dchk->tchk', context, w_xkv[0], preferred_element_type=F32).astype(BF16)
        xkv = jnp.transpose(xkv, (1, 2, 0, 3))
        return block_call((
            q, kv, kv_other, xkv, tokens, jnp.transpose(modulation, (1, 0, 2)),
            w_out[0].reshape(1280, D), jnp.transpose(w_xq[0], (1, 0, 2)), w_xout[0].reshape(1280, D),
            w_up[0], w_down[0], jnp.transpose(w_final)))

    in_specs = (P('sp', None), P(), P(), P(None, None, None, 'tp', None), P(None, 'tp', None, None),
                P(None, None, 'tp', None), P(None, None, None, 'tp', None), P(None, 'tp', None, None),
                P(None, None, 'tp'), P(None, 'tp', None), P())
    return jax.shard_map(device_step, mesh=mesh, in_specs=in_specs, out_specs=P('sp', None), check_vma=False)
```

```python
import functools
import jax
import jax.numpy as jnp
from jax import lax
from jax.experimental import pallas as pl
from jax.experimental.pallas import tpu as pltpu
from jax.sharding import PartitionSpec as P

F32 = jnp.float32
BF16 = jnp.bfloat16
LN_EPS = 1e-6
MESH = pl.DeviceIdType.MESH

W = 256
HD = 128
KD = 1280
NB = 5
KEYS = 512
D = 5120
ROWS = 256
NT = 20
KC = 4
HL = 10
NH = 2
RH = ROWS // NH
CB = RH // 2
OB = RH // 4
NSLOT = 40
HALVES = tuple(range(NH))
GA = 4
GD = 2
XC = 10
XR = 256 * 2 * HL


def dot(a, b):
    return jnp.dot(a, b, preferred_element_type=F32)


def dot_nt(a, b):
    return lax.dot_general(a, b, (((1,), (1,)), ((), ())), preferred_element_type=F32)


def block_kernel(tok_hbm, ctx_hbm, mod_ref, w_qkv, w_xkv, w_out, w_xq, w_xout, w_up, w_down, wf_hbm,
                 out_ref,
                 ring, part, dsum, xin, xres, hbuf, ubuf, qacc, obuf, kvs, kvx, xw, xf, cbuf, wf, obout,
                 rsem, lsem, xwsem, csem, ds_s, ds_r, xs_s, xs_r, ax_s, ax_r, ad_s, ad_r, af_s, af_r, ys_s, ys_r,
                 os_s, os_r):
    sp = lax.axis_index('sp')
    tp = lax.axis_index('tp')
    x = tp // 2
    c = tp % 2
    partner = (sp, 2 * x + (1 - c))
    across = (sp, 2 * (1 - x) + c)
    diagonal = (sp, 2 * (1 - x) + (1 - c))
    opposite = (1 - sp, tp)

    def kslice(kc):
        return pl.ds(kc * KD, KD)

    def nslice(nb):
        return pl.ds(nb * W, W)

    def start_cols(w, kc, nb, slot):
        pltpu.make_async_copy(w.at[kslice(kc), nslice(nb)], ring.at[slot], rsem.at[slot]).start()

    def start_heads(w, kc, b, slot):
        for hh in range(2):
            pltpu.make_async_copy(w.at[2 * b + hh, kslice(kc), :], ring.at[slot, :, pl.ds(HD * hh, HD)],
                                  rsem.at[slot]).start()

    def wait_block(slot):
        pltpu.make_async_copy(w_out.at[pl.ds(0, KD), pl.ds(0, W)], ring.at[slot], rsem.at[slot]).wait()

    def start_down(g, i, slot):
        start_cols(w_down, i % KC, NB * g + i // KC, slot)

    def tok_load(j):
        return pltpu.make_async_copy(tok_hbm.at[:, pl.ds(j * HD, HD)], kvx.at[j], lsem.at[j])

    def xw_load(i, slot):
        return pltpu.make_async_copy(w_xkv.at[pl.ds(i * 2 * XR, 2 * XR), :], xw.at[slot], xwsem.at[slot])

    def ctx_load(i, slot):
        return pltpu.make_async_copy(ctx_hbm.at[:, pl.ds(i * KEYS, KEYS)], cbuf.at[slot], csem.at[slot])

    wf_load = pltpu.make_async_copy(wf_hbm, wf, lsem.at[40])

    @pl.loop(0, 40)
    def _(j):
        tok_load(j).start()

    @pl.loop(0, NT)
    def _(i):
        start_heads(w_qkv.at[0], i // NB, i % NB, i)

    def kv_slot(kc):
        return (NT + HL * kc) % NSLOT

    def start_kv(kc):
        for m in range(2):
            for b in range(NB):
                start_heads(w_qkv.at[1 + m], kc, b, kv_slot(kc) + NB * m + b)

    start_kv(0)
    start_kv(1)

    barrier = pltpu.get_barrier_semaphore()
    for peer in (partner, across, diagonal, opposite):
        pl.semaphore_signal(barrier, inc=1, device_id=peer, device_id_type=MESH)

    scale = HD ** -0.5

    def attend(qh, k, v):
        s1 = dot_nt(qh, k[0:W, :]) * scale
        s2 = dot_nt(qh, k[W:KEYS, :]) * scale
        m = jnp.maximum(jnp.max(s1, axis=-1, keepdims=True), jnp.max(s2, axis=-1, keepdims=True))
        p1 = jnp.exp(s1 - m)
        p2 = jnp.exp(s2 - m)
        total = jnp.sum(p1, axis=-1, keepdims=True) + jnp.sum(p2, axis=-1, keepdims=True)
        o = dot(p1.astype(BF16), v[0:W, :]) + dot(p2.astype(BF16), v[W:KEYS, :])
        return (o / total).astype(BF16)

    def d2d(a, i, g):
        src = part.at[pl.ds(i * g, g), pl.ds(pl.multiple_of(a * RH + (1 - c) * CB, OB), CB), :]
        return pltpu.make_async_remote_copy(src_ref=src, dst_ref=dsum.at[a, pl.ds(i * g, g)], send_sem=ds_s.at[a, i],
                                            recv_sem=ds_r.at[a, i], device_id=partner, device_id_type=MESH)

    def xsend(a, i, g):
        src = dsum.at[a, pl.ds(i * g, g), pl.ds(pl.multiple_of((1 - x) * OB, OB), OB), :]
        return pltpu.make_async_remote_copy(src_ref=src, dst_ref=xin.at[a, pl.ds(i * g, g)], send_sem=xs_s.at[a, i],
                                            recv_sem=xs_r.at[a, i], device_id=across, device_id_type=MESH)

    def core_sum(a, i, g):
        d2d(a, i, g).wait_recv()
        for u in range(g):
            t = i * g + u
            dsum[a, t] = dsum[a, t] + part[t, pl.ds(pl.multiple_of(a * RH + c * CB, OB), CB), :]

    def rs_loop(compute, compute_halves, send_halves, g, lag):
        iters = NT // g

        @pl.loop(0, iters + lag)
        def _(i):
            @pl.when(i < iters)
            def _():
                compute(i)

            @pl.when(i >= lag)
            def _():
                for a in send_halves:
                    core_sum(a, i - lag, g)

            @pl.when(i < iters)
            def _():
                for a in compute_halves:
                    d2d(a, i, g).start()

            @pl.when(i >= lag)
            def _():
                for a in send_halves:
                    xsend(a, i - lag, g).start()

    def hrows(core, chip, a):
        return pl.ds(pl.multiple_of(a * RH + core * CB + chip * OB, OB), OB)

    def gather_copy(buf, kc, rows, ssem, rsem_, peer):
        ref = buf.at[pl.ds(kc * NB, NB), rows, :]
        return pltpu.make_async_remote_copy(src_ref=ref, dst_ref=ref, send_sem=ssem, recv_sem=rsem_,
                                            device_id=peer, device_id_type=MESH)

    def g_across(a, kc, chip, buf=hbuf):
        return gather_copy(buf, kc, hrows(c, chip, a), ax_s.at[a, kc], ax_r.at[a, kc], across)

    def g_partner(a, kc, core, buf=hbuf):
        return gather_copy(buf, kc, hrows(core, x, a), ad_s.at[a, kc], ad_r.at[a, kc], partner)

    def g_forward(a, kc, core, buf=hbuf):
        return gather_copy(buf, kc, hrows(core, 1 - x, a), af_s.at[a, kc], af_r.at[a, kc], partner)

    def modrow(r, t, width=W):
        return mod_ref[r, 0:1, pl.ds(pl.multiple_of(t * width, width), width)]

    def residual(a, gate, g, drained):
        def body(i, acc):
            xsend(a, i, g).wait()
            if not drained:
                d2d(a, i, g).wait_send()
            for u in range(g):
                t = i * g + u
                proj = (dsum[a, t, pl.ds(pl.multiple_of(x * OB, OB), OB), :] + xin[a, t]).astype(BF16).astype(F32)
                if gate is not None:
                    proj = modrow(gate, t) * proj
                new = xres[a, t] + proj
                xres[a, t] = new
                acc = acc + new
            return acc
        acc = lax.fori_loop(0, NT // g, body, jnp.zeros((OB, W), F32))
        return jnp.sum(acc, axis=-1, keepdims=True)

    def stats(a, row_sum):
        mean = row_sum / D

        def body(i, acc):
            for u in range(KC):
                d_ = xres[a, i * KC + u] - mean
                acc = acc + d_ * d_
            return acc
        acc = lax.fori_loop(0, NT // KC, body, jnp.zeros((OB, W), F32))
        var = jnp.sum(acc, axis=-1, keepdims=True) / D
        return mean, lax.rsqrt(var + LN_EPS)

    def norm_and_send(a, gate, drained, shift, gain):
        mean, inv = stats(a, residual(a, gate, GA, drained))

        @pl.loop(0, KC)
        def _(kc):
            for u in range(NB):
                t = kc * NB + u
                h = (xres[a, t] - mean) * inv
                if gain is not None:
                    h = h * (1.0 + modrow(gain, t)) + modrow(shift, t)
                hbuf[t, hrows(c, x, a), :] = h.astype(BF16)
            g_across(a, kc, x).start()
            g_partner(a, kc, c).start()

    def gather_forward(a, kc, buf=hbuf):
        g_across(a, kc, 1 - x, buf).wait_recv()
        g_forward(a, kc, c, buf).start()

    def gather_wait(a, kc, buf=hbuf):
        g_partner(a, kc, 1 - c, buf).wait_recv()
        g_forward(a, kc, 1 - c, buf).wait_recv()
        g_across(a, kc, x, buf).wait_send()
        g_partner(a, kc, c, buf).wait_send()
        g_forward(a, kc, c, buf).wait_send()

    def mm(lhs, slot):
        acc = dot(lhs(0), ring[slot, 0:W, :])
        for j in range(1, NB):
            acc = acc + dot(lhs(j), ring[slot, W * j:W * (j + 1), :])
        return acc

    def norm_tokens(r0, n, a):
        rows = pl.ds(pl.multiple_of(r0, OB), n)

        def sums(i, acc):
            for u in range(KC):
                acc = acc + kvx[i * KC + u, rows, :].astype(F32)
            return acc
        mean = jnp.sum(lax.fori_loop(0, HL, sums, jnp.zeros((n, HD), F32)), axis=-1, keepdims=True) / D

        def squares(i, acc):
            for u in range(KC):
                d_ = kvx[i * KC + u, rows, :].astype(F32) - mean
                acc = acc + d_ * d_
            return acc
        var = jnp.sum(lax.fori_loop(0, HL, squares, jnp.zeros((n, HD), F32)), axis=-1, keepdims=True) / D
        inv = lax.rsqrt(var + LN_EPS)

        @pl.loop(0, NT)
        def _(t):
            for hh in range(2):
                v = kvx[2 * t + hh, rows, :].astype(F32)
                if a is not None:
                    xres[a, t, :, HD * hh:HD * (hh + 1)] = v
                h = (v - mean) * inv * (1.0 + modrow(1, 2 * t + hh, HD)) + modrow(0, 2 * t + hh, HD)
                hbuf[t, rows, HD * hh:HD * (hh + 1)] = h.astype(BF16)

    def y_copy(a, kc):
        rows = hrows(c, x, a)
        return pltpu.make_async_remote_copy(
            src_ref=hbuf.at[pl.ds(kc * NB, NB), rows, :], dst_ref=ubuf.at[pl.ds(kc * NB, NB), rows, :],
            send_sem=ys_s.at[a, kc], recv_sem=ys_r.at[a, kc], device_id=opposite, device_id_type=MESH)

    def y_forward(kc):
        for a in HALVES:
            y_copy(a, kc).wait_recv()
            g_across(a, kc, x, ubuf).start()
            g_partner(a, kc, c, ubuf).start()

    def kv_step(buf, kc, half):
        first = kv_slot(kc)
        base = HL * half

        @pl.loop(0, 2)
        def _(m):
            if half == 0:
                for b in range(NB):
                    wait_block(first + NB * m + b)
            for b in range(NB):
                acc = mm(lambda j: buf[kc * NB + j], first + NB * m + b)
                if kc > 0:
                    acc = part[base + NB * m + b] + acc
                if kc < KC - 1:
                    part[base + NB * m + b] = acc
                else:
                    kvs[m, 2 * b, W * half:W * (half + 1), :] = acc[:, 0:HD].astype(BF16)
                    kvs[m, 2 * b + 1, W * half:W * (half + 1), :] = acc[:, HD:W].astype(BF16)

    with jax.named_scope("ln0"):
        @pl.loop(0, 40)
        def _(j):
            tok_load(j).wait()
        for a in HALVES:
            norm_tokens(a * RH + c * CB + x * OB, OB, a)
        pl.semaphore_wait(barrier, KC)
        for kc in range(KC):
            for a in HALVES:
                y_copy(a, kc).start()
        for a in HALVES:
            norm_tokens(a * RH + c * CB + (1 - x) * OB, OB, None)
            norm_tokens(a * RH + (1 - c) * CB, CB, None)

    with jax.named_scope("q"):
        for b in range(NB):
            qacc[b] = jnp.zeros((ROWS, W), F32)

        @pl.loop(0, KC)
        def _(kc):
            for b in range(NB):
                wait_block(kc * NB + b)
            for b in range(NB):
                qacc[b] += mm(lambda j: hbuf[kc * NB + j], kc * NB + b)
        start_kv(2)
        start_kv(3)

    for kc in range(KC):
        with jax.named_scope("kvfwd%d" % kc):
            y_forward(kc)
            if kc > 1:
                for a in HALVES:
                    gather_forward(a, kc - 2, ubuf)
        with jax.named_scope("kv%d" % kc):
            kv_step(hbuf, kc, 0)

    for kc in range(KC):
        with jax.named_scope("kvw%d" % kc):
            if kc < 2:
                for a in HALVES:
                    gather_forward(a, kc + 2, ubuf)
            for a in HALVES:
                gather_wait(a, kc, ubuf)
                y_copy(a, kc).wait_send()
        with jax.named_scope("kvo%d" % kc):
            kv_step(ubuf, kc, 1)
            for i in range(HL):
                if kc < 2:
                    start_cols(w_out, 0, HL * kc + i, kv_slot(kc) + i)
                else:
                    j = HL * (kc - 2) + i
                    start_heads(w_xq, j // NB, j % NB, kv_slot(kc) + i)

    wf_load.start()
    for i in range(2):
        xw_load(i, i).start()
        ctx_load(i, i).start()

    with jax.named_scope("attn1"):
        @pl.loop(0, HL // 2)
        def _(b):
            for hh in range(2):
                for a in HALVES:
                    rows = pl.ds(a * RH, RH)
                    qh = qacc[b, rows, HD * hh:HD * (hh + 1)].astype(BF16)
                    obuf[b, rows, HD * hh:HD * (hh + 1)] = attend(qh, kvs.at[0, 2 * b + hh], kvs.at[1, 2 * b + hh])

    def out_tiles(i):
        for u in range(GA):
            wait_block(NT + i * GA + u)
        for u in range(GA):
            part[i * GA + u] = mm(lambda j: obuf[j], NT + i * GA + u)
        for u in range(GA):
            start_cols(w_xout, 0, i * GA + u, NT + i * GA + u)

    with jax.named_scope("rs1A"):
        rs_loop(out_tiles, HALVES, HALVES[:1], GA, 2)
    with jax.named_scope("rs1B"):
        for a in HALVES[1:]:
            @pl.loop(0, NT // GA)
            def _(i):
                core_sum(a, i, GA)
                xsend(a, i, GA).start()
        for a in HALVES:
            @pl.loop(0, NT // GA)
            def _(i):
                d2d(a, i, GA).wait_send()

    def text_kv(lo, hi):
        @pl.loop(lo, hi)
        def _(i):
            slot = i % 2
            xw_load(i, slot).wait()
            for q in range(2):
                @pl.loop(0, XR // W)
                def _(r):
                    xf[q, pl.ds(pl.multiple_of(r * W, W), W), :] = (
                        xw[slot, pl.ds(pl.multiple_of(q * XR + r * W, W), W), :].astype(F32))

            @pl.when(i < XC - 2)
            def _():
                xw_load(i + 2, slot).start()
            ctx_load(i, slot).wait()

            @pl.loop(0, HL // 2)
            def _(b):
                for hh in range(2):
                    h = 2 * b + hh
                    top, low = part[2 * h], part[2 * h + 1]
                    for q in range(2):
                        w = jnp.concatenate([xf[q, pl.ds(2 * h, W, stride=NT), :],
                                             xf[q, pl.ds(2 * h + 1, W, stride=NT), :]], axis=1).astype(BF16)
                        top = top + dot(cbuf[slot, 0:W, W * q:W * (q + 1)], w)
                        low = low + dot(cbuf[slot, W:KEYS, W * q:W * (q + 1)], w)
                    part[2 * h] = top
                    part[2 * h + 1] = low

            @pl.when(i < XC - 2)
            def _():
                ctx_load(i + 2, slot).start()

    with jax.named_scope("xkv_a"):
        @pl.loop(0, NT)
        def _(t):
            part[t] = jnp.zeros((W, W), F32)
        text_kv(0, 6)
    wf_load.wait()
    with jax.named_scope("fin1_0"):
        norm_and_send(0, 2, True, None, None)
    with jax.named_scope("xkv_b"):
        text_kv(6, XC)

        @pl.loop(0, NT)
        def _(t):
            kvx[t] = part[t, :, 0:HD].astype(BF16)
            kvx[NT + t] = part[t, :, HD:W].astype(BF16)
    for a in HALVES[1:]:
        with jax.named_scope("fin1_%d" % a):
            norm_and_send(a, 2, True, None, None)

    def attend2(qh, h):
        s1 = dot_nt(qh, kvx[2 * h]) * scale
        s2 = dot_nt(qh, kvx[2 * h + 1]) * scale
        m = jnp.maximum(jnp.max(s1, axis=-1, keepdims=True), jnp.max(s2, axis=-1, keepdims=True))
        p1 = jnp.exp(s1 - m)
        p2 = jnp.exp(s2 - m)
        total = jnp.sum(p1, axis=-1, keepdims=True) + jnp.sum(p2, axis=-1, keepdims=True)
        o = dot(p1.astype(BF16), kvx[NT + 2 * h]) + dot(p2.astype(BF16), kvx[NT + 2 * h + 1])
        return (o / total).astype(BF16)

    for a in HALVES:
        rows = pl.ds(a * RH, RH)
        last = a == HALVES[-1]
        for b in range(NB):
            qacc[b, rows, :] = jnp.zeros((RH, W), F32)

        gather_forward(a, 0)

        @pl.loop(0, KC)
        def _(kc):
            @pl.when(kc < KC - 1)
            def _():
                gather_forward(a, kc + 1)
            gather_wait(a, kc)
            if a == 0:
                for b in range(NB):
                    wait_block(kc * NB + b)
            for b in range(NB):
                qacc[b, rows, :] += mm(lambda j: hbuf[kc * NB + j, rows, :], kc * NB + b)
            if last:
                for b in range(NB):
                    start_cols(w_up, 0, kc * NB + b, kc * NB + b)

        @pl.loop(0, HL // 2)
        def _(b):
            for hh in range(2):
                qh = qacc[b, rows, HD * hh:HD * (hh + 1)].astype(BF16)
                obuf[b, rows, HD * hh:HD * (hh + 1)] = attend2(qh, 2 * b + hh)

        def xout_tiles(i):
            if a == 0:
                for u in range(GA):
                    wait_block(NT + i * GA + u)
            for u in range(GA):
                part[i * GA + u, rows, :] = mm(lambda j: obuf[j, rows, :], NT + i * GA + u)
            if last:
                for u in range(GA):
                    start_cols(w_up, 1, i * GA + u, NT + i * GA + u)

        with jax.named_scope("rs2_%d" % a):
            rs_loop(xout_tiles, (a,), (a,), GA, 2)

    for a in HALVES:
        with jax.named_scope("fin2_%d" % a):
            norm_and_send(a, None, False, 3, KC)

    for a in HALVES[:-1]:
        @pl.loop(0, KC)
        def _(kc):
            gather_forward(a, kc)
    gather_forward(HALVES[-1], 0)
    for kc in range(KC):
        if kc < KC - 1:
            gather_forward(HALVES[-1], kc + 1)
        for a in HALVES:
            gather_wait(a, kc)
        base = 0 if kc % 2 == 0 else NT

        scope = jax.named_scope("up%d" % kc)
        scope.__enter__()

        @pl.loop(0, NT // KC)
        def _(i):
            for u in range(KC):
                wait_block(base + i * KC + u)
            for u in range(KC):
                nb = i * KC + u
                acc = mm(lambda j: hbuf[kc * NB + j], base + nb)
                if kc > 0:
                    acc = part[nb] + acc
                if kc < KC - 1:
                    part[nb] = acc
                else:
                    ubuf[nb] = jax.nn.gelu(acc, approximate=True).astype(BF16)
            for u in range(KC):
                nb = i * KC + u
                if kc < 2:
                    start_cols(w_up, kc + 2, nb, base + nb)
                else:
                    start_down(kc - 2, nb, base + nb)
        scope.__exit__(None, None, None)

    def down_tiles(i):
        def slot(t, kc):
            return NT * (t // NB % 2) + KC * (t % NB) + kc

        for u in range(GD):
            for kc in range(KC):
                wait_block(slot(i * GD + u, kc))
        for u in range(GD):
            t = i * GD + u
            acc = mm(lambda j: ubuf[j], slot(t, 0))
            for kc in range(1, KC):
                acc = acc + mm(lambda j: ubuf[NB * kc + j], slot(t, kc))
            part[t] = acc
        for u in range(GD):
            t = i * GD + u

            @pl.when(t < HL)
            def _():
                for kc in range(KC):
                    start_cols(w_down, kc, t + HL, slot(t, kc))

    with jax.named_scope("down"):
        rs_loop(down_tiles, HALVES, HALVES, GD, 1)

    def out_copy(a, peer, k, core, chip):
        ref = obout.at[hrows(core, chip, a), :]
        return pltpu.make_async_remote_copy(src_ref=ref, dst_ref=ref, send_sem=os_s.at[a, k], recv_sem=os_r.at[a, k],
                                            device_id=peer, device_id_type=MESH)

    for a in HALVES:
        mean, inv = stats(a, residual(a, NB, GD, False))

        def body(i, acc):
            for u in range(KC):
                t = i * KC + u
                fin = ((xres[a, t] - mean) * inv).astype(BF16)
                acc = acc + dot_nt(fin, wf[:, pl.ds(pl.multiple_of(t * W, W), W)])
            return acc
        acc = lax.fori_loop(0, NT // KC, body, jnp.zeros((OB, 64), F32))
        obout[hrows(c, x, a), :] = jnp.concatenate([acc, jnp.zeros((OB, 64), F32)], axis=1)
        out_copy(a, across, 0, c, x).start()
        out_copy(a, partner, 1, c, x).start()
        out_copy(a, diagonal, 2, c, x).start()
    for a in HALVES:
        out_copy(a, across, 0, c, 1 - x).wait()
        out_copy(a, partner, 1, 1 - c, x).wait()
        out_copy(a, diagonal, 2, 1 - c, 1 - x).wait()
    out_ref[...] = obout[:, 0:64]


def block_call(args):
    any_spec = pl.BlockSpec(memory_space=pl.ANY)
    vmem_spec = pl.BlockSpec(memory_space=pltpu.VMEM)
    sem = pltpu.SemaphoreType.DMA
    return pl.pallas_call(
        block_kernel,
        out_shape=jax.ShapeDtypeStruct((ROWS, 64), F32),
        in_specs=[any_spec] * 2 + [vmem_spec] + [any_spec] * 8,
        out_specs=vmem_spec,
        scratch_shapes=[
            pltpu.VMEM((NSLOT, KD, W), BF16),
            pltpu.VMEM((NT, ROWS, W), F32),
            pltpu.VMEM((NH, NT, CB, W), F32),
            pltpu.VMEM((NH, NT, OB, W), F32),
            pltpu.VMEM((NH, NT, OB, W), F32),
            pltpu.VMEM((NT, ROWS, W), BF16),
            pltpu.VMEM((NT, ROWS, W), BF16),
            pltpu.VMEM((NB, ROWS, W), F32),
            pltpu.VMEM((NB, ROWS, W), BF16),
            pltpu.VMEM((2, HL, KEYS, HD), BF16),
            pltpu.VMEM((2 * NT, W, HD), BF16),
            pltpu.VMEM((2, 2 * XR, HD), BF16),
            pltpu.VMEM((2, XR, HD), F32),
            pltpu.VMEM((2, KEYS, KEYS), BF16),
            pltpu.VMEM((64, D), BF16),
            pltpu.VMEM((ROWS, HD), F32),
            sem((NSLOT,)), sem((41,)), sem((2,)), sem((2,)),
            sem((NH, NT)), sem((NH, NT)), sem((NH, NT)), sem((NH, NT)),
            sem((NH, KC)), sem((NH, KC)), sem((NH, KC)), sem((NH, KC)), sem((NH, KC)), sem((NH, KC)),
            sem((NH, KC)), sem((NH, KC)),
            sem((NH, 3)), sem((NH, 3)),
        ],
        compiler_params=pltpu.CompilerParams(collective_id=0, has_side_effects=True, vmem_limit_bytes=67_000_000),
        cost_estimate=pl.CostEstimate(flops=60 * 10**9, bytes_accessed=218 * 10**6, transcendentals=4 * 10**6),
        name='dit_block',
    )(*args)


def solution(mesh):
    def device_step(tokens, context, modulation, w_qkv, w_out, w_xq, w_xkv, w_xout, w_up, w_down, w_final):
        return block_call((
            tokens, context, jnp.transpose(modulation, (1, 0, 2)),
            jnp.transpose(w_qkv[0], (1, 2, 0, 3)), jnp.transpose(w_xkv[0], (0, 2, 1, 3)).reshape(2 * HL * D, HD),
            w_out[0].reshape(KD, D), jnp.transpose(w_xq[0], (1, 0, 2)), w_xout[0].reshape(KD, D),
            w_up[0], w_down[0], jnp.transpose(w_final)))

    in_specs = (P('sp', None), P(), P(), P(None, None, None, 'tp', None), P(None, 'tp', None, None),
                P(None, None, 'tp', None), P(None, None, None, 'tp', None), P(None, 'tp', None, None),
                P(None, None, 'tp'), P(None, 'tp', None), P())
    return jax.shard_map(device_step, mesh=mesh, in_specs=in_specs, out_specs=P('sp', None), check_vma=False)
```

```python
import functools
import jax
import jax.numpy as jnp
from jax import lax
from jax.experimental import pallas as pl
from jax.experimental.pallas import tpu as pltpu
from jax.sharding import PartitionSpec as P

F32 = jnp.float32
BF16 = jnp.bfloat16
LN_EPS = 1e-6
MESH = pl.DeviceIdType.MESH

W = 256
HD = 128
KD = 1280
NB = 5
KEYS = 512
D = 5120
ROWS = 256
NT = 20
KC = 4
HL = 10
NH = 2
RH = ROWS // NH
CB = RH // 2
OB = RH // 4
NSLOT = 40
HALVES = tuple(range(NH))
GA = 4
XC = 10
XR = 256 * 2 * HL


def dot(a, b):
    return jnp.dot(a, b, preferred_element_type=F32)


def dot_nt(a, b):
    return lax.dot_general(a, b, (((1,), (1,)), ((), ())), preferred_element_type=F32)


def block_kernel(tok_hbm, ctx_hbm, mod_ref, w_qkv, w_xkv, w_out, w_xq, w_xout, w_up, w_down, wf_hbm,
                 out_ref,
                 ring, part, dsum, xin, xres, hbuf, ubuf, qacc, obuf, kvs, kvx, xw, xf, cbuf, wf, obout,
                 rsem, lsem, xwsem, csem, ds_s, ds_r, xs_s, xs_r, ax_s, ax_r, ad_s, ad_r, af_s, af_r, ys_s, ys_r,
                 os_s, os_r):
    sp = lax.axis_index('sp')
    tp = lax.axis_index('tp')
    x = tp // 2
    c = tp % 2
    partner = (sp, 2 * x + (1 - c))
    across = (sp, 2 * (1 - x) + c)
    diagonal = (sp, 2 * (1 - x) + (1 - c))
    opposite = (1 - sp, tp)

    def kslice(kc):
        return pl.ds(kc * KD, KD)

    def nslice(nb):
        return pl.ds(nb * W, W)

    def start_cols(w, kc, nb, slot):
        pltpu.make_async_copy(w.at[kslice(kc), nslice(nb)], ring.at[slot], rsem.at[slot]).start()

    def start_heads(w, kc, b, slot):
        for hh in range(2):
            pltpu.make_async_copy(w.at[2 * b + hh, kslice(kc), :], ring.at[slot, :, pl.ds(HD * hh, HD)],
                                  rsem.at[slot]).start()

    def wait_block(slot):
        pltpu.make_async_copy(w_out.at[pl.ds(0, KD), pl.ds(0, W)], ring.at[slot], rsem.at[slot]).wait()

    def start_down(g, i, slot):
        start_cols(w_down, i % KC, NB * g + i // KC, slot)

    def tok_load(j):
        return pltpu.make_async_copy(tok_hbm.at[:, pl.ds(j * HD, HD)], kvx.at[j], lsem.at[j])

    def xw_load(i, slot):
        return pltpu.make_async_copy(w_xkv.at[pl.ds(i * 2 * XR, 2 * XR), :], xw.at[slot], xwsem.at[slot])

    def ctx_load(i, slot):
        return pltpu.make_async_copy(ctx_hbm.at[:, pl.ds(i * KEYS, KEYS)], cbuf.at[slot], csem.at[slot])

    wf_load = pltpu.make_async_copy(wf_hbm, wf, lsem.at[40])

    @pl.loop(0, 40)
    def _(j):
        tok_load(j).start()

    def kv_slot(kc):
        return (NT + HL * kc) % NSLOT

    def start_kv(kc):
        for m in range(2):
            for b in range(NB):
                start_heads(w_qkv.at[1 + m], kc, b, kv_slot(kc) + NB * m + b)

    barrier = pltpu.get_barrier_semaphore()
    for peer in (partner, across, diagonal, opposite):
        pl.semaphore_signal(barrier, inc=1, device_id=peer, device_id_type=MESH)

    scale = HD ** -0.5

    def attend(qh, k, v):
        s1 = dot_nt(qh, k[0:W, :]) * scale
        s2 = dot_nt(qh, k[W:KEYS, :]) * scale
        m = jnp.maximum(jnp.max(s1, axis=-1, keepdims=True), jnp.max(s2, axis=-1, keepdims=True))
        p1 = jnp.exp(s1 - m)
        p2 = jnp.exp(s2 - m)
        total = jnp.sum(p1, axis=-1, keepdims=True) + jnp.sum(p2, axis=-1, keepdims=True)
        o = dot(p1.astype(BF16), v[0:W, :]) + dot(p2.astype(BF16), v[W:KEYS, :])
        return (o / total).astype(BF16)

    def d2d(a, i, g):
        src = part.at[pl.ds(i * g, g), pl.ds(pl.multiple_of(a * RH + (1 - c) * CB, OB), CB), :]
        return pltpu.make_async_remote_copy(src_ref=src, dst_ref=dsum.at[a, pl.ds(i * g, g)], send_sem=ds_s.at[a, i],
                                            recv_sem=ds_r.at[a, i], device_id=partner, device_id_type=MESH)

    def xsend(a, i, g):
        src = dsum.at[a, pl.ds(i * g, g), pl.ds(pl.multiple_of((1 - x) * OB, OB), OB), :]
        return pltpu.make_async_remote_copy(src_ref=src, dst_ref=xin.at[a, pl.ds(i * g, g)], send_sem=xs_s.at[a, i],
                                            recv_sem=xs_r.at[a, i], device_id=across, device_id_type=MESH)

    def core_sum(a, i, g):
        d2d(a, i, g).wait_recv()
        for u in range(g):
            t = i * g + u
            dsum[a, t] = dsum[a, t] + part[t, pl.ds(pl.multiple_of(a * RH + c * CB, OB), CB), :]

    def rs_loop(compute, compute_halves, send_halves, g, lag):
        iters = NT // g

        @pl.loop(0, iters + lag)
        def _(i):
            @pl.when(i < iters)
            def _():
                compute(i)

            @pl.when(i >= lag)
            def _():
                for a in send_halves:
                    core_sum(a, i - lag, g)

            @pl.when(i < iters)
            def _():
                for a in compute_halves:
                    d2d(a, i, g).start()

            @pl.when(i >= lag)
            def _():
                for a in send_halves:
                    xsend(a, i - lag, g).start()

    def hrows(core, chip, a):
        return pl.ds(pl.multiple_of(a * RH + core * CB + chip * OB, OB), OB)

    def gather_copy(buf, kc, rows, ssem, rsem_, peer):
        ref = buf.at[pl.ds(kc * NB, NB), rows, :]
        return pltpu.make_async_remote_copy(src_ref=ref, dst_ref=ref, send_sem=ssem, recv_sem=rsem_,
                                            device_id=peer, device_id_type=MESH)

    def g_across(a, kc, chip, buf=hbuf):
        return gather_copy(buf, kc, hrows(c, chip, a), ax_s.at[a, kc], ax_r.at[a, kc], across)

    def g_partner(a, kc, core, buf=hbuf):
        return gather_copy(buf, kc, hrows(core, x, a), ad_s.at[a, kc], ad_r.at[a, kc], partner)

    def g_forward(a, kc, core, buf=hbuf):
        return gather_copy(buf, kc, hrows(core, 1 - x, a), af_s.at[a, kc], af_r.at[a, kc], partner)

    def modrow(r, t, width=W):
        return mod_ref[r, 0:1, pl.ds(pl.multiple_of(t * width, width), width)]

    def residual(a, gate, drained):
        g = GA
        def body(i, acc):
            xsend(a, i, g).wait()
            if not drained:
                d2d(a, i, g).wait_send()
            for u in range(g):
                t = i * g + u
                proj = (dsum[a, t, pl.ds(pl.multiple_of(x * OB, OB), OB), :] + xin[a, t]).astype(BF16).astype(F32)
                if gate is not None:
                    proj = modrow(gate, t) * proj
                new = xres[a, t] + proj
                xres[a, t] = new
                acc = acc + new
            return acc
        acc = lax.fori_loop(0, NT // g, body, jnp.zeros((OB, W), F32))
        return jnp.sum(acc, axis=-1, keepdims=True)

    def stats(a, row_sum):
        mean = row_sum / D

        def body(i, acc):
            for u in range(KC):
                d_ = xres[a, i * KC + u] - mean
                acc = acc + d_ * d_
            return acc
        acc = lax.fori_loop(0, NT // KC, body, jnp.zeros((OB, W), F32))
        var = jnp.sum(acc, axis=-1, keepdims=True) / D
        return mean, lax.rsqrt(var + LN_EPS)

    def norm_and_send(a, gate, drained, shift, gain):
        mean, inv = stats(a, residual(a, gate, drained))

        @pl.loop(0, KC)
        def _(kc):
            for u in range(NB):
                t = kc * NB + u
                h = (xres[a, t] - mean) * inv
                if gain is not None:
                    h = h * (1.0 + modrow(gain, t)) + modrow(shift, t)
                hbuf[t, hrows(c, x, a), :] = h.astype(BF16)
            g_across(a, kc, x).start()
            g_partner(a, kc, c).start()

    def gather_forward(a, kc, buf=hbuf):
        g_across(a, kc, 1 - x, buf).wait_recv()
        g_forward(a, kc, c, buf).start()

    def gather_wait(a, kc, buf=hbuf):
        g_partner(a, kc, 1 - c, buf).wait_recv()
        g_forward(a, kc, 1 - c, buf).wait_recv()
        g_across(a, kc, x, buf).wait_send()
        g_partner(a, kc, c, buf).wait_send()
        g_forward(a, kc, c, buf).wait_send()

    def mm(lhs, slot):
        acc = dot(lhs(0), ring[slot, 0:W, :])
        for j in range(1, NB):
            acc = acc + dot(lhs(j), ring[slot, W * j:W * (j + 1), :])
        return acc

    def norm_tokens(blocks):
        spans = [pl.ds(pl.multiple_of(r0, OB), n) for r0, n, _ in blocks]
        zeros = tuple(jnp.zeros((n, HD), F32) for _, n, _ in blocks)

        def across_lanes(accs):
            return [jnp.sum(acc, axis=-1, keepdims=True) / D for acc in accs]

        def sums(i, accs):
            for u in range(4):
                accs = tuple(acc + kvx[i * 4 + u, r, :].astype(F32) for acc, r in zip(accs, spans))
            return accs
        means = across_lanes(lax.fori_loop(0, HL, sums, zeros))

        def squares(i, accs):
            for u in range(4):
                ds = [kvx[i * 4 + u, r, :].astype(F32) - mean for r, mean in zip(spans, means)]
                accs = tuple(acc + d_ * d_ for acc, d_ in zip(accs, ds))
            return accs
        invs = [lax.rsqrt(var + LN_EPS) for var in across_lanes(lax.fori_loop(0, HL, squares, zeros))]

        @pl.loop(0, NT)
        def _(t):
            for hh in range(2):
                gain = 1.0 + modrow(1, 2 * t + hh, HD)
                shift = modrow(0, 2 * t + hh, HD)
                lanes = pl.ds(HD * hh, HD)
                for (_, _, a), r, mean, inv in zip(blocks, spans, means, invs):
                    v = kvx[2 * t + hh, r, :].astype(F32)
                    if a is not None:
                        xres[a, t, :, lanes] = v
                    hbuf[t, r, lanes] = ((v - mean) * inv * gain + shift).astype(BF16)

    def y_copy(a, kc):
        rows = hrows(c, x, a)
        return pltpu.make_async_remote_copy(
            src_ref=hbuf.at[pl.ds(kc * NB, NB), rows, :], dst_ref=ubuf.at[pl.ds(kc * NB, NB), rows, :],
            send_sem=ys_s.at[a, kc], recv_sem=ys_r.at[a, kc], device_id=opposite, device_id_type=MESH)

    def y_forward(kc):
        for a in HALVES:
            y_copy(a, kc).wait_recv()
            g_across(a, kc, x, ubuf).start()
            g_partner(a, kc, c, ubuf).start()

    def kv_step(buf, kc, half):
        first = kv_slot(kc)
        base = HL * half

        @pl.loop(0, 2)
        def _(m):
            if half == 0:
                for b in range(NB):
                    wait_block(first + NB * m + b)
            for b in range(NB):
                acc = mm(lambda j: buf[kc * NB + j], first + NB * m + b)
                if kc > 0:
                    acc = part[base + NB * m + b] + acc
                if kc < KC - 1:
                    part[base + NB * m + b] = acc
                else:
                    kvs[m, 2 * b, W * half:W * (half + 1), :] = acc[:, 0:HD].astype(BF16)
                    kvs[m, 2 * b + 1, W * half:W * (half + 1), :] = acc[:, HD:W].astype(BF16)

    with jax.named_scope("ln0"):
        @pl.loop(0, 40)
        def _(j):
            tok_load(j).wait()
        @pl.loop(0, NT)
        def _(i):
            start_heads(w_qkv.at[0], i // NB, i % NB, i)

        start_kv(0)
        start_kv(1)
        norm_tokens([(a * RH + c * CB + x * OB, OB, a) for a in HALVES])
        pl.semaphore_wait(barrier, KC)
        for kc in range(KC):
            for a in HALVES:
                y_copy(a, kc).start()
        norm_tokens([(a * RH + c * CB + (1 - x) * OB, OB, None) for a in HALVES]
                    + [(a * RH + (1 - c) * CB, CB, None) for a in HALVES])

    with jax.named_scope("q"):
        for b in range(NB):
            qacc[b] = jnp.zeros((ROWS, W), F32)

        @pl.loop(0, KC)
        def _(kc):
            for b in range(NB):
                wait_block(kc * NB + b)
            for b in range(NB):
                qacc[b] += mm(lambda j: hbuf[kc * NB + j], kc * NB + b)
        start_kv(2)
        start_kv(3)

    for kc in range(KC):
        with jax.named_scope("kvfwd%d" % kc):
            y_forward(kc)
            if kc > 1:
                for a in HALVES:
                    gather_forward(a, kc - 2, ubuf)
        with jax.named_scope("kv%d" % kc):
            kv_step(hbuf, kc, 0)

    for kc in range(KC):
        with jax.named_scope("kvw%d" % kc):
            if kc < 2:
                for a in HALVES:
                    gather_forward(a, kc + 2, ubuf)
            for a in HALVES:
                gather_wait(a, kc, ubuf)
                y_copy(a, kc).wait_send()
        with jax.named_scope("kvo%d" % kc):
            kv_step(ubuf, kc, 1)
            for i in range(HL):
                if kc < 2:
                    start_cols(w_out, 0, HL * kc + i, kv_slot(kc) + i)
                else:
                    j = HL * (kc - 2) + i
                    start_heads(w_xq, j // NB, j % NB, kv_slot(kc) + i)

    wf_load.start()
    for i in range(2):
        xw_load(i, i).start()
        ctx_load(i, i).start()

    for a in HALVES:
        rows = pl.ds(a * RH, RH)
        with jax.named_scope("attn1_%d" % a):
            @pl.loop(0, HL // 2)
            def _(b):
                for hh in range(2):
                    h = 2 * b + hh
                    lanes = pl.ds(HD * hh, HD)
                    obuf[b, rows, lanes] = attend(qacc[b, rows, lanes].astype(BF16), kvs.at[0, h], kvs.at[1, h])

        def out_tiles(i):
            if a == 0:
                for u in range(GA):
                    wait_block(NT + i * GA + u)
            for u in range(GA):
                part[i * GA + u, rows, :] = mm(lambda j: obuf[j, rows, :], NT + i * GA + u)
            if a == HALVES[-1]:
                for u in range(GA):
                    start_cols(w_xout, 0, i * GA + u, NT + i * GA + u)

        with jax.named_scope("rs1_%d" % a):
            rs_loop(out_tiles, (a,), (a,), GA, 2)
    for a in HALVES:
        @pl.loop(0, NT // GA)
        def _(i):
            d2d(a, i, GA).wait_send()

    def text_kv(lo, hi):
        @pl.loop(lo, hi)
        def _(i):
            slot = i % 2
            xw_load(i, slot).wait()
            for q in range(2):
                @pl.loop(0, XR // W)
                def _(r):
                    xf[q, pl.ds(pl.multiple_of(r * W, W), W), :] = (
                        xw[slot, pl.ds(pl.multiple_of(q * XR + r * W, W), W), :].astype(F32))

            @pl.when(i < XC - 2)
            def _():
                xw_load(i + 2, slot).start()
            ctx_load(i, slot).wait()

            @pl.loop(0, HL // 2)
            def _(b):
                for hh in range(2):
                    h = 2 * b + hh
                    top, low = part[2 * h], part[2 * h + 1]
                    for q in range(2):
                        w = jnp.concatenate([xf[q, pl.ds(2 * h, W, stride=NT), :],
                                             xf[q, pl.ds(2 * h + 1, W, stride=NT), :]], axis=1).astype(BF16)
                        top = top + dot(cbuf[slot, 0:W, W * q:W * (q + 1)], w)
                        low = low + dot(cbuf[slot, W:KEYS, W * q:W * (q + 1)], w)
                    part[2 * h] = top
                    part[2 * h + 1] = low

            @pl.when(i < XC - 2)
            def _():
                ctx_load(i + 2, slot).start()

    with jax.named_scope("xkv_a"):
        @pl.loop(0, NT)
        def _(t):
            part[t] = jnp.zeros((W, W), F32)
        text_kv(0, 6)
    wf_load.wait()
    with jax.named_scope("fin1_0"):
        norm_and_send(0, 2, True, None, None)
    with jax.named_scope("xkv_b"):
        text_kv(6, XC)

        @pl.loop(0, NT)
        def _(t):
            kvx[t] = part[t, :, 0:HD].astype(BF16)
            kvx[NT + t] = part[t, :, HD:W].astype(BF16)
    for a in HALVES[1:]:
        with jax.named_scope("fin1_%d" % a):
            norm_and_send(a, 2, True, None, None)

    def attend2(qh, h):
        s1 = dot_nt(qh, kvx[2 * h]) * scale
        s2 = dot_nt(qh, kvx[2 * h + 1]) * scale
        m = jnp.maximum(jnp.max(s1, axis=-1, keepdims=True), jnp.max(s2, axis=-1, keepdims=True))
        p1 = jnp.exp(s1 - m)
        p2 = jnp.exp(s2 - m)
        total = jnp.sum(p1, axis=-1, keepdims=True) + jnp.sum(p2, axis=-1, keepdims=True)
        o = dot(p1.astype(BF16), kvx[NT + 2 * h]) + dot(p2.astype(BF16), kvx[NT + 2 * h + 1])
        return (o / total).astype(BF16)

    for a in HALVES:
        rows = pl.ds(a * RH, RH)
        last = a == HALVES[-1]
        for b in range(NB):
            qacc[b, rows, :] = jnp.zeros((RH, W), F32)

        gather_forward(a, 0)

        @pl.loop(0, KC)
        def _(kc):
            @pl.when(kc < KC - 1)
            def _():
                gather_forward(a, kc + 1)
            gather_wait(a, kc)
            if a == 0:
                for b in range(NB):
                    wait_block(kc * NB + b)
            for b in range(NB):
                qacc[b, rows, :] += mm(lambda j: hbuf[kc * NB + j, rows, :], kc * NB + b)
            if last:
                for b in range(NB):
                    start_cols(w_up, 0, kc * NB + b, kc * NB + b)

        @pl.loop(0, HL // 2)
        def _(b):
            for hh in range(2):
                qh = qacc[b, rows, HD * hh:HD * (hh + 1)].astype(BF16)
                obuf[b, rows, HD * hh:HD * (hh + 1)] = attend2(qh, 2 * b + hh)

        def xout_tiles(i):
            if a == 0:
                for u in range(GA):
                    wait_block(NT + i * GA + u)
            for u in range(GA):
                part[i * GA + u, rows, :] = mm(lambda j: obuf[j, rows, :], NT + i * GA + u)
            if last:
                for u in range(GA):
                    start_cols(w_up, 1, i * GA + u, NT + i * GA + u)

        with jax.named_scope("rs2_%d" % a):
            rs_loop(xout_tiles, (a,), (a,), GA, 2)

    for a in HALVES:
        with jax.named_scope("fin2_%d" % a):
            norm_and_send(a, None, False, 3, KC)

    def up_step(kc, rows, refill):
        base = NT * (kc % 2)

        @pl.loop(0, NT // 4)
        def _(i):
            if rows != 1:
                for u in range(4):
                    wait_block(base + i * 4 + u)
            for u in range(4):
                nb = i * 4 + u
                r = pl.ds(0, ROWS) if rows is None else pl.ds(rows * RH, RH)
                acc = mm(lambda j: hbuf[kc * NB + j, r, :], base + nb)
                if kc > 0:
                    acc = part[nb, r, :] + acc
                if kc < KC - 1:
                    part[nb, r, :] = acc
                else:
                    ubuf[nb] = jax.nn.gelu(acc, approximate=True).astype(BF16)
            if refill:
                for u in range(4):
                    nb = i * 4 + u
                    if kc < 2:
                        start_cols(w_up, kc + 2, nb, base + nb)
                    else:
                        start_down(kc - 2, nb, base + nb)

    for a in HALVES:
        for kc in range(2):
            gather_forward(a, 2 * kc)
            gather_forward(a, 2 * kc + 1)
            gather_wait(a, kc)
            with jax.named_scope("up%d_%d" % (kc, a)):
                up_step(kc, a, a == HALVES[-1])
    for kc in range(2, KC):
        for a in HALVES:
            gather_wait(a, kc)
        with jax.named_scope("up%d" % kc):
            up_step(kc, None, True)

    def xsend_both(t):
        src = dsum.at[:, t, pl.ds(pl.multiple_of((1 - x) * OB, OB), OB), :]
        return pltpu.make_async_remote_copy(src_ref=src, dst_ref=xin.at[:, t], send_sem=xs_s.at[0, t],
                                            recv_sem=xs_r.at[0, t], device_id=across, device_id_type=MESH)

    def down_slot(t, kc):
        return NT * (t // NB % 2) + KC * (t % NB) + kc

    with jax.named_scope("down"):
        @pl.loop(0, NT + 1)
        def _(t):
            @pl.when(t < NT)
            def _():
                for kc in range(KC):
                    wait_block(down_slot(t, kc))
                acc = mm(lambda j: ubuf[j], down_slot(t, 0))
                for kc in range(1, KC):
                    acc = acc + mm(lambda j: ubuf[NB * kc + j], down_slot(t, kc))
                part[t] = acc

            @pl.when(t < HL)
            def _():
                for kc in range(KC):
                    start_cols(w_down, kc, t + HL, down_slot(t, kc))

            @pl.when(t > 0)
            def _():
                for a in HALVES:
                    core_sum(a, t - 1, 1)

            @pl.when(t < NT)
            def _():
                for a in HALVES:
                    d2d(a, t, 1).start()

            @pl.when(t > 0)
            def _():
                xsend_both(t - 1).start()

    def out_copy(a, peer, k, core, chip):
        ref = obout.at[hrows(core, chip, a), :]
        return pltpu.make_async_remote_copy(src_ref=ref, dst_ref=ref, send_sem=os_s.at[a, k], recv_sem=os_r.at[a, k],
                                            device_id=peer, device_id_type=MESH)

    with jax.named_scope("last_sum"):
        def last_residual(t, accs):
            xsend_both(t).wait()
            news = []
            for a in HALVES:
                d2d(a, t, 1).wait_send()
                proj = dsum[a, t, pl.ds(pl.multiple_of(x * OB, OB), OB), :] + xin[a, t]
                new = xres[a, t] + modrow(NB, t) * proj.astype(BF16).astype(F32)
                xres[a, t] = new
                news.append(new)
            return tuple(acc + new for acc, new in zip(accs, news))
        zeros = tuple(jnp.zeros((OB, W), F32) for a in HALVES)
        sums = lax.fori_loop(0, NT, last_residual, zeros)
    with jax.named_scope("last_norm"):
        means = [jnp.sum(acc, axis=-1, keepdims=True) / D for acc in sums]

        def squares(i, accs):
            for u in range(4):
                ds = [xres[a, i * 4 + u] - means[a] for a in HALVES]
                accs = tuple(acc + d_ * d_ for acc, d_ in zip(accs, ds))
            return accs
        invs = [lax.rsqrt(jnp.sum(acc, axis=-1, keepdims=True) / D + LN_EPS)
                for acc in lax.fori_loop(0, NT // 4, squares, zeros)]

        def project(i, acc):
            for u in range(4):
                t = i * 4 + u
                fin = jnp.concatenate([(xres[a, t] - means[a]) * invs[a] for a in HALVES], axis=0).astype(BF16)
                acc = acc + dot_nt(fin, wf[:, pl.ds(pl.multiple_of(t * W, W), W)])
            return acc
        acc = lax.fori_loop(0, NT // 4, project, jnp.zeros((NH * OB, 64), F32))
        acc = jnp.concatenate([acc, jnp.zeros((NH * OB, 64), F32)], axis=1)
        for a in HALVES:
            obout[hrows(c, x, a), :] = acc[a * OB:(a + 1) * OB, :]
            out_copy(a, across, 0, c, x).start()
            out_copy(a, partner, 1, c, x).start()
            out_copy(a, diagonal, 2, c, x).start()
    for a in HALVES:
        out_copy(a, across, 0, c, 1 - x).wait()
        out_copy(a, partner, 1, 1 - c, x).wait()
        out_copy(a, diagonal, 2, 1 - c, 1 - x).wait()
    out_ref[...] = obout[:, 0:64]


def block_call(args):
    any_spec = pl.BlockSpec(memory_space=pl.ANY)
    vmem_spec = pl.BlockSpec(memory_space=pltpu.VMEM)
    sem = pltpu.SemaphoreType.DMA
    return pl.pallas_call(
        block_kernel,
        out_shape=jax.ShapeDtypeStruct((ROWS, 64), F32),
        in_specs=[any_spec] * 2 + [vmem_spec] + [any_spec] * 8,
        out_specs=vmem_spec,
        scratch_shapes=[
            pltpu.VMEM((NSLOT, KD, W), BF16),
            pltpu.VMEM((NT, ROWS, W), F32),
            pltpu.VMEM((NH, NT, CB, W), F32),
            pltpu.VMEM((NH, NT, OB, W), F32),
            pltpu.VMEM((NH, NT, OB, W), F32),
            pltpu.VMEM((NT, ROWS, W), BF16),
            pltpu.VMEM((NT, ROWS, W), BF16),
            pltpu.VMEM((NB, ROWS, W), F32),
            pltpu.VMEM((NB, ROWS, W), BF16),
            pltpu.VMEM((2, HL, KEYS, HD), BF16),
            pltpu.VMEM((2 * NT, W, HD), BF16),
            pltpu.VMEM((2, 2 * XR, HD), BF16),
            pltpu.VMEM((2, XR, HD), F32),
            pltpu.VMEM((2, KEYS, KEYS), BF16),
            pltpu.VMEM((64, D), BF16),
            pltpu.VMEM((ROWS, HD), F32),
            sem((NSLOT,)), sem((41,)), sem((2,)), sem((2,)),
            sem((NH, NT)), sem((NH, NT)), sem((NH, NT)), sem((NH, NT)),
            sem((NH, KC)), sem((NH, KC)), sem((NH, KC)), sem((NH, KC)), sem((NH, KC)), sem((NH, KC)),
            sem((NH, KC)), sem((NH, KC)),
            sem((NH, 3)), sem((NH, 3)),
        ],
        compiler_params=pltpu.CompilerParams(collective_id=0, has_side_effects=True, vmem_limit_bytes=67_000_000),
        cost_estimate=pl.CostEstimate(flops=60 * 10**9, bytes_accessed=218 * 10**6, transcendentals=4 * 10**6),
        name='dit_block',
    )(*args)


def solution(mesh):
    def device_step(tokens, context, modulation, w_qkv, w_out, w_xq, w_xkv, w_xout, w_up, w_down, w_final):
        return block_call((
            tokens, context, jnp.transpose(modulation, (1, 0, 2)),
            jnp.transpose(w_qkv[0], (1, 2, 0, 3)), jnp.transpose(w_xkv[0], (0, 2, 1, 3)).reshape(2 * HL * D, HD),
            w_out[0].reshape(KD, D), jnp.transpose(w_xq[0], (1, 0, 2)), w_xout[0].reshape(KD, D),
            w_up[0], w_down[0], jnp.transpose(w_final)))

    in_specs = (P('sp', None), P(), P(), P(None, None, None, 'tp', None), P(None, 'tp', None, None),
                P(None, None, 'tp', None), P(None, None, None, 'tp', None), P(None, 'tp', None, None),
                P(None, None, 'tp'), P(None, 'tp', None), P())
    return jax.shard_map(device_step, mesh=mesh, in_specs=in_specs, out_specs=P('sp', None), check_vma=False)
```

```python
import functools
import jax
import jax.numpy as jnp
from jax import lax
from jax.experimental import pallas as pl
from jax.experimental.pallas import tpu as pltpu
from jax.sharding import PartitionSpec as P

F32 = jnp.float32
BF16 = jnp.bfloat16
LN_EPS = 1e-6
MESH = pl.DeviceIdType.MESH

W = 256
HD = 128
KD = 1280
NB = 5
KEYS = 512
D = 5120
ROWS = 256
NT = 20
KC = 4
HL = 10
NH = 2
RH = ROWS // NH
CB = RH // 2
OB = RH // 4
NSLOT = 40
HALVES = tuple(range(NH))
GA = 4
XC = 10
XR = 256 * 2 * HL


def dot(a, b):
    return jnp.dot(a, b, preferred_element_type=F32)


def dot_nt(a, b):
    return lax.dot_general(a, b, (((1,), (1,)), ((), ())), preferred_element_type=F32)


def block_kernel(tok_hbm, ctx_hbm, mod_ref, w_qkv, w_xkv, w_out, w_xq, w_xout, w_up, w_down, wf_hbm,
                 out_ref,
                 ring, part, dsum, xin, xres, hbuf, ubuf, qacc, obuf, kvs, kvx, xw, xf, cbuf, wf, obout,
                 rsem, lsem, xwsem, csem, ds_s, ds_r, xs_s, xs_r, ax_s, ax_r, ad_s, ad_r, af_s, af_r, ys_s, ys_r,
                 os_s, os_r):
    sp = lax.axis_index('sp')
    tp = lax.axis_index('tp')
    x = tp // 2
    c = tp % 2
    partner = (sp, 2 * x + (1 - c))
    across = (sp, 2 * (1 - x) + c)
    diagonal = (sp, 2 * (1 - x) + (1 - c))
    opposite = (1 - sp, tp)

    def kslice(kc):
        return pl.ds(kc * KD, KD)

    def nslice(nb):
        return pl.ds(nb * W, W)

    def start_cols(w, kc, nb, slot):
        pltpu.make_async_copy(w.at[kslice(kc), nslice(nb)], ring.at[slot], rsem.at[slot]).start()

    def start_heads(w, kc, b, slot):
        for hh in range(2):
            pltpu.make_async_copy(w.at[2 * b + hh, kslice(kc), :], ring.at[slot, :, pl.ds(HD * hh, HD)],
                                  rsem.at[slot]).start()

    def wait_block(slot):
        pltpu.make_async_copy(w_out.at[pl.ds(0, KD), pl.ds(0, W)], ring.at[slot], rsem.at[slot]).wait()

    def start_down(g, i, slot):
        start_cols(w_down, i % KC, NB * g + i // KC, slot)

    def tok_load(j):
        return pltpu.make_async_copy(tok_hbm.at[:, pl.ds(j * HD, HD)], kvx.at[j], lsem.at[j])

    def xw_load(i, slot):
        return pltpu.make_async_copy(w_xkv.at[pl.ds(i * 2 * XR, 2 * XR), :], xw.at[slot], xwsem.at[slot])

    def ctx_load(i, slot):
        return pltpu.make_async_copy(ctx_hbm.at[:, pl.ds(i * KEYS, KEYS)], cbuf.at[slot], csem.at[slot])

    wf_load = pltpu.make_async_copy(wf_hbm, wf, lsem.at[40])

    @pl.loop(0, 40)
    def _(j):
        tok_load(j).start()

    def kv_slot(kc):
        return (NT + HL * kc) % NSLOT

    def start_kv(kc):
        for m in range(2):
            for b in range(NB):
                start_heads(w_qkv.at[1 + m], kc, b, kv_slot(kc) + NB * m + b)

    barrier = pltpu.get_barrier_semaphore()
    for peer in (partner, across, diagonal, opposite):
        pl.semaphore_signal(barrier, inc=1, device_id=peer, device_id_type=MESH)

    scale = HD ** -0.5

    def attend(a, keys, values):
        rows = pl.ds(a * RH, RH)
        for h in range(HL):
            lanes = pl.ds(HD * (h % 2), HD)
            qh = qacc[h // 2, rows, lanes].astype(BF16)
            s1, s2 = [dot_nt(qh, k) * scale for k in keys(h)]
            m = jnp.max(jnp.maximum(s1, s2), axis=-1, keepdims=True)
            p1 = jnp.exp(s1 - m)
            p2 = jnp.exp(s2 - m)
            total = jnp.sum(p1 + p2, axis=-1, keepdims=True)
            v1, v2 = values(h)
            o = dot(p1.astype(BF16), v1) + dot(p2.astype(BF16), v2)
            obuf[h // 2, rows, lanes] = (o / total).astype(BF16)

    def d2d(a, i, g):
        src = part.at[pl.ds(i * g, g), pl.ds(pl.multiple_of(a * RH + (1 - c) * CB, OB), CB), :]
        return pltpu.make_async_remote_copy(src_ref=src, dst_ref=dsum.at[a, pl.ds(i * g, g)], send_sem=ds_s.at[a, i],
                                            recv_sem=ds_r.at[a, i], device_id=partner, device_id_type=MESH)

    def xsend(a, i, g):
        src = dsum.at[a, pl.ds(i * g, g), pl.ds(pl.multiple_of((1 - x) * OB, OB), OB), :]
        return pltpu.make_async_remote_copy(src_ref=src, dst_ref=xin.at[a, pl.ds(i * g, g)], send_sem=xs_s.at[a, i],
                                            recv_sem=xs_r.at[a, i], device_id=across, device_id_type=MESH)

    def core_sum(a, i, g):
        d2d(a, i, g).wait_recv()
        for u in range(g):
            t = i * g + u
            dsum[a, t] = dsum[a, t] + part[t, pl.ds(pl.multiple_of(a * RH + c * CB, OB), CB), :]

    def rs_loop(compute, compute_halves, send_halves, g, lag):
        iters = NT // g

        @pl.loop(0, iters + lag)
        def _(i):
            @pl.when(i < iters)
            def _():
                compute(i)

            @pl.when(i >= lag)
            def _():
                for a in send_halves:
                    core_sum(a, i - lag, g)

            @pl.when(i < iters)
            def _():
                for a in compute_halves:
                    d2d(a, i, g).start()

            @pl.when(i >= lag)
            def _():
                for a in send_halves:
                    xsend(a, i - lag, g).start()

    def hrows(core, chip, a):
        return pl.ds(pl.multiple_of(a * RH + core * CB + chip * OB, OB), OB)

    def gather_copy(buf, kc, rows, ssem, rsem_, peer):
        ref = buf.at[pl.ds(kc * NB, NB), rows, :]
        return pltpu.make_async_remote_copy(src_ref=ref, dst_ref=ref, send_sem=ssem, recv_sem=rsem_,
                                            device_id=peer, device_id_type=MESH)

    def g_across(a, kc, chip, buf=hbuf):
        return gather_copy(buf, kc, hrows(c, chip, a), ax_s.at[a, kc], ax_r.at[a, kc], across)

    def g_partner(a, kc, core, buf=hbuf):
        return gather_copy(buf, kc, hrows(core, x, a), ad_s.at[a, kc], ad_r.at[a, kc], partner)

    def g_forward(a, kc, core, buf=hbuf):
        return gather_copy(buf, kc, hrows(core, 1 - x, a), af_s.at[a, kc], af_r.at[a, kc], partner)

    def modrow(r, t, width=W):
        return mod_ref[r, 0:1, pl.ds(pl.multiple_of(t * width, width), width)]

    def residual(a, gate, drained):
        g = GA
        def body(i, acc):
            xsend(a, i, g).wait()
            if not drained:
                d2d(a, i, g).wait_send()
            for u in range(g):
                t = i * g + u
                proj = (dsum[a, t, pl.ds(pl.multiple_of(x * OB, OB), OB), :] + xin[a, t]).astype(BF16).astype(F32)
                if gate is not None:
                    proj = modrow(gate, t) * proj
                new = xres[a, t] + proj
                xres[a, t] = new
                acc = acc + new
            return acc
        acc = lax.fori_loop(0, NT // g, body, jnp.zeros((OB, W), F32))
        return jnp.sum(acc, axis=-1, keepdims=True)

    def stats(a, row_sum):
        mean = row_sum / D

        def body(i, acc):
            for u in range(KC):
                d_ = xres[a, i * KC + u] - mean
                acc = acc + d_ * d_
            return acc
        acc = lax.fori_loop(0, NT // KC, body, jnp.zeros((OB, W), F32))
        var = jnp.sum(acc, axis=-1, keepdims=True) / D
        return mean, lax.rsqrt(var + LN_EPS)

    def norm_and_send(a, gate, drained, shift, gain):
        mean, inv = stats(a, residual(a, gate, drained))

        @pl.loop(0, KC)
        def _(kc):
            for u in range(NB):
                t = kc * NB + u
                h = (xres[a, t] - mean) * inv
                if gain is not None:
                    h = h * (1.0 + modrow(gain, t)) + modrow(shift, t)
                hbuf[t, hrows(c, x, a), :] = h.astype(BF16)
            g_across(a, kc, x).start()
            g_partner(a, kc, c).start()

    def gather_forward(a, kc, buf=hbuf):
        g_across(a, kc, 1 - x, buf).wait_recv()
        g_forward(a, kc, c, buf).start()

    def gather_wait(a, kc, buf=hbuf):
        g_partner(a, kc, 1 - c, buf).wait_recv()
        g_forward(a, kc, 1 - c, buf).wait_recv()
        g_across(a, kc, x, buf).wait_send()
        g_partner(a, kc, c, buf).wait_send()
        g_forward(a, kc, c, buf).wait_send()

    def mm(lhs, slot):
        acc = dot(lhs(0), ring[slot, 0:W, :])
        for j in range(1, NB):
            acc = acc + dot(lhs(j), ring[slot, W * j:W * (j + 1), :])
        return acc

    def norm_tokens(blocks):
        spans = [pl.ds(pl.multiple_of(r0, OB), n) for r0, n, _ in blocks]
        zeros = tuple(jnp.zeros((n, HD), F32) for _, n, _ in blocks)

        def across_lanes(accs):
            return [jnp.sum(acc, axis=-1, keepdims=True) / D for acc in accs]

        def sums(i, accs):
            for u in range(4):
                accs = tuple(acc + kvx[i * 4 + u, r, :].astype(F32) for acc, r in zip(accs, spans))
            return accs
        means = across_lanes(lax.fori_loop(0, HL, sums, zeros))

        def squares(i, accs):
            for u in range(4):
                ds = [kvx[i * 4 + u, r, :].astype(F32) - mean for r, mean in zip(spans, means)]
                accs = tuple(acc + d_ * d_ for acc, d_ in zip(accs, ds))
            return accs
        invs = [lax.rsqrt(var + LN_EPS) for var in across_lanes(lax.fori_loop(0, HL, squares, zeros))]

        @pl.loop(0, NT)
        def _(t):
            for hh in range(2):
                gain = 1.0 + modrow(1, 2 * t + hh, HD)
                shift = modrow(0, 2 * t + hh, HD)
                lanes = pl.ds(HD * hh, HD)
                for (_, _, a), r, mean, inv in zip(blocks, spans, means, invs):
                    v = kvx[2 * t + hh, r, :].astype(F32)
                    if a is not None:
                        xres[a, t, :, lanes] = v
                    hbuf[t, r, lanes] = ((v - mean) * inv * gain + shift).astype(BF16)

    def y_copy(a, kc):
        rows = hrows(c, x, a)
        return pltpu.make_async_remote_copy(
            src_ref=hbuf.at[pl.ds(kc * NB, NB), rows, :], dst_ref=ubuf.at[pl.ds(kc * NB, NB), rows, :],
            send_sem=ys_s.at[a, kc], recv_sem=ys_r.at[a, kc], device_id=opposite, device_id_type=MESH)

    def y_forward(kc):
        for a in HALVES:
            y_copy(a, kc).wait_recv()
            g_across(a, kc, x, ubuf).start()
            g_partner(a, kc, c, ubuf).start()

    def kv_step(buf, kc, half):
        first = kv_slot(kc)
        base = HL * half

        @pl.loop(0, 2)
        def _(m):
            if half == 0:
                for b in range(NB):
                    wait_block(first + NB * m + b)
            for b in range(NB):
                acc = mm(lambda j: buf[kc * NB + j], first + NB * m + b)
                if kc > 0:
                    acc = part[base + NB * m + b] + acc
                if kc < KC - 1:
                    part[base + NB * m + b] = acc
                else:
                    kvs[m, 2 * b, W * half:W * (half + 1), :] = acc[:, 0:HD].astype(BF16)
                    kvs[m, 2 * b + 1, W * half:W * (half + 1), :] = acc[:, HD:W].astype(BF16)

    with jax.named_scope("ln0"):
        @pl.loop(0, 40)
        def _(j):
            tok_load(j).wait()
        @pl.loop(0, NT)
        def _(i):
            start_heads(w_qkv.at[0], i // NB, i % NB, i)

        start_kv(0)
        start_kv(1)
        norm_tokens([(a * RH + c * CB + x * OB, OB, a) for a in HALVES])
        pl.semaphore_wait(barrier, KC)
        for kc in range(KC):
            for a in HALVES:
                y_copy(a, kc).start()
        norm_tokens([(a * RH + c * CB + (1 - x) * OB, OB, None) for a in HALVES]
                    + [(a * RH + (1 - c) * CB, CB, None) for a in HALVES])

    with jax.named_scope("q"):
        for b in range(NB):
            qacc[b] = jnp.zeros((ROWS, W), F32)

        @pl.loop(0, KC)
        def _(kc):
            for b in range(NB):
                wait_block(kc * NB + b)
            for b in range(NB):
                qacc[b] += mm(lambda j: hbuf[kc * NB + j], kc * NB + b)
        start_kv(2)
        start_kv(3)

    def spread(kc):
        for a in HALVES:
            gather_forward(a, kc, ubuf)

    def other_kv(kc):
        for a in HALVES:
            gather_wait(a, kc, ubuf)
            y_copy(a, kc).wait_send()
        kv_step(ubuf, kc, 1)
        for i in range(HL):
            if kc < 2:
                start_cols(w_out, 0, HL * kc + i, kv_slot(kc) + i)
            else:
                j = HL * (kc - 2) + i
                start_heads(w_xq, j // NB, j % NB, kv_slot(kc) + i)

    with jax.named_scope("kv"):
        y_forward(0)
        kv_step(hbuf, 0, 0)
        kv_step(hbuf, 1, 0)
        y_forward(1)
        kv_step(hbuf, 2, 0)
        spread(0)
        y_forward(2)
        kv_step(hbuf, 3, 0)
        spread(1)
    with jax.named_scope("kvo"):
        other_kv(0)
        y_forward(3)
        other_kv(1)
        spread(2)
        other_kv(2)
        spread(3)
        other_kv(3)

    wf_load.start()
    for i in range(2):
        xw_load(i, i).start()
        ctx_load(i, i).start()

    for a in HALVES:
        rows = pl.ds(a * RH, RH)
        with jax.named_scope("attn1_%d" % a):
            attend(a, lambda h: [kvs[0, h, 0:W, :], kvs[0, h, W:2 * W, :]],
                   lambda h: [kvs[1, h, 0:W, :], kvs[1, h, W:2 * W, :]])

        def out_tiles(i):
            if a == 0:
                for u in range(GA):
                    wait_block(NT + i * GA + u)
            for u in range(GA):
                part[i * GA + u, rows, :] = mm(lambda j: obuf[j, rows, :], NT + i * GA + u)
            if a == HALVES[-1]:
                for u in range(GA):
                    start_cols(w_xout, 0, i * GA + u, NT + i * GA + u)

        with jax.named_scope("rs1_%d" % a):
            rs_loop(out_tiles, (a,), (a,), GA, 2)
    for a in HALVES:
        @pl.loop(0, NT // GA)
        def _(i):
            d2d(a, i, GA).wait_send()

    def text_kv(lo, hi):
        @pl.loop(lo, hi)
        def _(i):
            slot = i % 2
            xw_load(i, slot).wait()
            for q in range(2):
                @pl.loop(0, XR // W)
                def _(r):
                    xf[q, pl.ds(pl.multiple_of(r * W, W), W), :] = (
                        xw[slot, pl.ds(pl.multiple_of(q * XR + r * W, W), W), :].astype(F32))

            @pl.when(i < XC - 2)
            def _():
                xw_load(i + 2, slot).start()
            ctx_load(i, slot).wait()

            @pl.loop(0, HL // 2)
            def _(b):
                for hh in range(2):
                    h = 2 * b + hh
                    top, low = part[2 * h], part[2 * h + 1]
                    for q in range(2):
                        w = jnp.concatenate([xf[q, pl.ds(2 * h, W, stride=NT), :],
                                             xf[q, pl.ds(2 * h + 1, W, stride=NT), :]], axis=1).astype(BF16)
                        top = top + dot(cbuf[slot, 0:W, W * q:W * (q + 1)], w)
                        low = low + dot(cbuf[slot, W:KEYS, W * q:W * (q + 1)], w)
                    part[2 * h] = top
                    part[2 * h + 1] = low

            @pl.when(i < XC - 2)
            def _():
                ctx_load(i + 2, slot).start()

    with jax.named_scope("xkv_a"):
        @pl.loop(0, NT)
        def _(t):
            part[t] = jnp.zeros((W, W), F32)
        text_kv(0, 6)
    wf_load.wait()
    with jax.named_scope("fin1_0"):
        norm_and_send(0, 2, True, None, None)
    with jax.named_scope("xkv_b"):
        text_kv(6, 8)
    for a in HALVES[1:]:
        with jax.named_scope("fin1_%d" % a):
            norm_and_send(a, 2, True, None, None)
    with jax.named_scope("xkv_c"):
        text_kv(8, XC)

        @pl.loop(0, NT)
        def _(t):
            kvx[t] = part[t, :, 0:HD].astype(BF16)
            kvx[NT + t] = part[t, :, HD:W].astype(BF16)

    for a in HALVES:
        rows = pl.ds(a * RH, RH)
        last = a == HALVES[-1]
        for b in range(NB):
            qacc[b, rows, :] = jnp.zeros((RH, W), F32)

        gather_forward(a, 0)

        @pl.loop(0, KC)
        def _(kc):
            @pl.when(kc < KC - 1)
            def _():
                gather_forward(a, kc + 1)
            gather_wait(a, kc)
            if a == 0:
                for b in range(NB):
                    wait_block(kc * NB + b)
            for b in range(NB):
                qacc[b, rows, :] += mm(lambda j: hbuf[kc * NB + j, rows, :], kc * NB + b)
            if last:
                for b in range(NB):
                    start_cols(w_up, 0, kc * NB + b, kc * NB + b)

        with jax.named_scope("attn2_%d" % a):
            attend(a, lambda h: [kvx[2 * h], kvx[2 * h + 1]], lambda h: [kvx[NT + 2 * h], kvx[NT + 2 * h + 1]])

        def xout_tiles(i):
            if a == 0:
                for u in range(GA):
                    wait_block(NT + i * GA + u)
            for u in range(GA):
                part[i * GA + u, rows, :] = mm(lambda j: obuf[j, rows, :], NT + i * GA + u)
            if last:
                for u in range(GA):
                    start_cols(w_up, 1, i * GA + u, NT + i * GA + u)

        with jax.named_scope("rs2_%d" % a):
            rs_loop(xout_tiles, (a,), (a,), GA, 2)

    for a in HALVES:
        with jax.named_scope("fin2_%d" % a):
            norm_and_send(a, None, False, 3, KC)

    def up_step(kc, rows, refill):
        base = NT * (kc % 2)

        @pl.loop(0, NT // 4)
        def _(i):
            if rows != 1:
                for u in range(4):
                    wait_block(base + i * 4 + u)
            for u in range(4):
                nb = i * 4 + u
                r = pl.ds(0, ROWS) if rows is None else pl.ds(rows * RH, RH)
                acc = mm(lambda j: hbuf[kc * NB + j, r, :], base + nb)
                if kc > 0:
                    acc = part[nb, r, :] + acc
                if kc < KC - 1:
                    part[nb, r, :] = acc
                else:
                    ubuf[nb] = jax.nn.gelu(acc, approximate=True).astype(BF16)
            if refill:
                for u in range(4):
                    nb = i * 4 + u
                    if kc < 2:
                        start_cols(w_up, kc + 2, nb, base + nb)
                    else:
                        start_down(kc - 2, nb, base + nb)

    for a in HALVES:
        for kc in range(2):
            gather_forward(a, 2 * kc)
            gather_forward(a, 2 * kc + 1)
            gather_wait(a, kc)
            with jax.named_scope("up%d_%d" % (kc, a)):
                up_step(kc, a, a == HALVES[-1])
    for kc in range(2, KC):
        for a in HALVES:
            gather_wait(a, kc)
        with jax.named_scope("up%d" % kc):
            up_step(kc, None, True)

    def xsend_both(t):
        src = dsum.at[:, t, pl.ds(pl.multiple_of((1 - x) * OB, OB), OB), :]
        return pltpu.make_async_remote_copy(src_ref=src, dst_ref=xin.at[:, t], send_sem=xs_s.at[0, t],
                                            recv_sem=xs_r.at[0, t], device_id=across, device_id_type=MESH)

    def down_slot(t, kc):
        return NT * (t // NB % 2) + KC * (t % NB) + kc

    with jax.named_scope("down"):
        @pl.loop(0, NT + 1)
        def _(t):
            @pl.when(t < NT)
            def _():
                for kc in range(KC):
                    wait_block(down_slot(t, kc))
                acc = mm(lambda j: ubuf[j], down_slot(t, 0))
                for kc in range(1, KC):
                    acc = acc + mm(lambda j: ubuf[NB * kc + j], down_slot(t, kc))
                part[t] = acc

            @pl.when(t < HL)
            def _():
                for kc in range(KC):
                    start_cols(w_down, kc, t + HL, down_slot(t, kc))

            @pl.when(t > 0)
            def _():
                for a in HALVES:
                    core_sum(a, t - 1, 1)

            @pl.when(t < NT)
            def _():
                for a in HALVES:
                    d2d(a, t, 1).start()

            @pl.when(t > 0)
            def _():
                xsend_both(t - 1).start()

    def out_copy(a, peer, k, core, chip):
        ref = obout.at[hrows(core, chip, a), :]
        return pltpu.make_async_remote_copy(src_ref=ref, dst_ref=ref, send_sem=os_s.at[a, k], recv_sem=os_r.at[a, k],
                                            device_id=peer, device_id_type=MESH)

    with jax.named_scope("last_sum"):
        def last_residual(t, accs):
            xsend_both(t).wait()
            news = []
            for a in HALVES:
                d2d(a, t, 1).wait_send()
                proj = dsum[a, t, pl.ds(pl.multiple_of(x * OB, OB), OB), :] + xin[a, t]
                new = xres[a, t] + modrow(NB, t) * proj.astype(BF16).astype(F32)
                xres[a, t] = new
                news.append(new)
            return tuple(acc + new for acc, new in zip(accs, news))
        zeros = tuple(jnp.zeros((OB, W), F32) for a in HALVES)
        sums = lax.fori_loop(0, NT, last_residual, zeros)
    with jax.named_scope("last_norm"):
        means = [jnp.sum(acc, axis=-1, keepdims=True) / D for acc in sums]

        def squares(i, accs):
            for u in range(4):
                ds = [xres[a, i * 4 + u] - means[a] for a in HALVES]
                accs = tuple(acc + d_ * d_ for acc, d_ in zip(accs, ds))
            return accs
        invs = [lax.rsqrt(jnp.sum(acc, axis=-1, keepdims=True) / D + LN_EPS)
                for acc in lax.fori_loop(0, NT // 4, squares, zeros)]

        def project(i, acc):
            for u in range(4):
                t = i * 4 + u
                fin = jnp.concatenate([(xres[a, t] - means[a]) * invs[a] for a in HALVES], axis=0).astype(BF16)
                acc = acc + dot_nt(fin, wf[:, pl.ds(pl.multiple_of(t * W, W), W)])
            return acc
        acc = lax.fori_loop(0, NT // 4, project, jnp.zeros((NH * OB, 64), F32))
        acc = jnp.concatenate([acc, jnp.zeros((NH * OB, 64), F32)], axis=1)
        for a in HALVES:
            obout[hrows(c, x, a), :] = acc[a * OB:(a + 1) * OB, :]
            out_copy(a, across, 0, c, x).start()
            out_copy(a, partner, 1, c, x).start()
            out_copy(a, diagonal, 2, c, x).start()
    for a in HALVES:
        out_copy(a, across, 0, c, 1 - x).wait()
        out_copy(a, partner, 1, 1 - c, x).wait()
        out_copy(a, diagonal, 2, 1 - c, 1 - x).wait()
    out_ref[...] = jnp.transpose(obout[...])[0:64, :]


def block_call(args):
    any_spec = pl.BlockSpec(memory_space=pl.ANY)
    vmem_spec = pl.BlockSpec(memory_space=pltpu.VMEM)
    sem = pltpu.SemaphoreType.DMA
    return pl.pallas_call(
        block_kernel,
        out_shape=jax.ShapeDtypeStruct((64, ROWS), F32),
        in_specs=[any_spec] * 2 + [vmem_spec] + [any_spec] * 8,
        out_specs=vmem_spec,
        scratch_shapes=[
            pltpu.VMEM((NSLOT, KD, W), BF16),
            pltpu.VMEM((NT, ROWS, W), F32),
            pltpu.VMEM((NH, NT, CB, W), F32),
            pltpu.VMEM((NH, NT, OB, W), F32),
            pltpu.VMEM((NH, NT, OB, W), F32),
            pltpu.VMEM((NT, ROWS, W), BF16),
            pltpu.VMEM((NT, ROWS, W), BF16),
            pltpu.VMEM((NB, ROWS, W), F32),
            pltpu.VMEM((NB, ROWS, W), BF16),
            pltpu.VMEM((2, HL, KEYS, HD), BF16),
            pltpu.VMEM((2 * NT, W, HD), BF16),
            pltpu.VMEM((2, 2 * XR, HD), BF16),
            pltpu.VMEM((2, XR, HD), F32),
            pltpu.VMEM((2, KEYS, KEYS), BF16),
            pltpu.VMEM((64, D), BF16),
            pltpu.VMEM((ROWS, HD), F32),
            sem((NSLOT,)), sem((41,)), sem((2,)), sem((2,)),
            sem((NH, NT)), sem((NH, NT)), sem((NH, NT)), sem((NH, NT)),
            sem((NH, KC)), sem((NH, KC)), sem((NH, KC)), sem((NH, KC)), sem((NH, KC)), sem((NH, KC)),
            sem((NH, KC)), sem((NH, KC)),
            sem((NH, 3)), sem((NH, 3)),
        ],
        compiler_params=pltpu.CompilerParams(collective_id=0, has_side_effects=True, vmem_limit_bytes=67_000_000),
        cost_estimate=pl.CostEstimate(flops=60 * 10**9, bytes_accessed=218 * 10**6, transcendentals=4 * 10**6),
        name='dit_block',
    )(*args)


def solution(mesh):
    def device_step(tokens, context, modulation, w_qkv, w_out, w_xq, w_xkv, w_xout, w_up, w_down, w_final):
        return jnp.transpose(block_call((
            tokens, context, jnp.transpose(modulation, (1, 0, 2)),
            jnp.transpose(w_qkv[0], (1, 2, 0, 3)), jnp.transpose(w_xkv[0], (0, 2, 1, 3)).reshape(2 * HL * D, HD),
            w_out[0].reshape(KD, D), jnp.transpose(w_xq[0], (1, 0, 2)), w_xout[0].reshape(KD, D),
            w_up[0], w_down[0], jnp.transpose(w_final))))

    in_specs = (P('sp', None), P(), P(), P(None, None, None, 'tp', None), P(None, 'tp', None, None),
                P(None, None, 'tp', None), P(None, None, None, 'tp', None), P(None, 'tp', None, None),
                P(None, None, 'tp'), P(None, 'tp', None), P())
    return jax.shard_map(device_step, mesh=mesh, in_specs=in_specs, out_specs=P('sp', None), check_vma=False)
```

```python
import functools
import jax
import jax.numpy as jnp
from jax import lax
from jax.experimental import pallas as pl
from jax.experimental.pallas import tpu as pltpu
from jax.sharding import PartitionSpec as P

F32 = jnp.float32
BF16 = jnp.bfloat16
LN_EPS = 1e-6
MESH = pl.DeviceIdType.MESH

W = 256
HD = 128
KD = 1280
NB = 5
KEYS = 512
D = 5120
ROWS = 256
NT = 20
KC = 4
HL = 10
NH = 2
RH = ROWS // NH
CB = RH // 2
OB = RH // 4
NSLOT = 40
HALVES = tuple(range(NH))
UP = 10
GA = 4
XC = 10
XR = 256 * 2 * HL


def dot(a, b):
    return jnp.dot(a, b, preferred_element_type=F32)


def dot_nt(a, b):
    return lax.dot_general(a, b, (((1,), (1,)), ((), ())), preferred_element_type=F32)


def block_kernel(tok_hbm, ctx_hbm, mod_ref, w_qkv, w_xkv, w_out, w_xq, w_xout, w_up, w_down, wf_hbm,
                 out_ref,
                 ring, part, dsum, xin, xres, hbuf, ubuf, qacc, obuf, kvs, kvx, xw, xf, cbuf, wf, obout,
                 rsem, lsem, xwsem, csem, ds_s, ds_r, xs_s, xs_r, ax_s, ax_r, ad_s, ad_r, af_s, af_r, ys_s, ys_r,
                 os_s, os_r):
    sp = lax.axis_index('sp')
    tp = lax.axis_index('tp')
    x = tp // 2
    c = tp % 2
    partner = (sp, 2 * x + (1 - c))
    across = (sp, 2 * (1 - x) + c)
    diagonal = (sp, 2 * (1 - x) + (1 - c))
    opposite = (1 - sp, tp)

    def kslice(kc):
        return pl.ds(kc * KD, KD)

    def nslice(nb):
        return pl.ds(nb * W, W)

    def start_cols(w, kc, nb, slot):
        pltpu.make_async_copy(w.at[kslice(kc), nslice(nb)], ring.at[slot], rsem.at[slot]).start()

    def start_heads(w, kc, b, slot):
        for hh in range(2):
            pltpu.make_async_copy(w.at[2 * b + hh, kslice(kc), :], ring.at[slot, :, pl.ds(HD * hh, HD)],
                                  rsem.at[slot]).start()

    def wait_block(slot):
        pltpu.make_async_copy(w_out.at[pl.ds(0, KD), pl.ds(0, W)], ring.at[slot], rsem.at[slot]).wait()

    def start_down(g, i, slot):
        start_cols(w_down, i % KC, NB * g + i // KC, slot)

    def tok_load(j):
        return pltpu.make_async_copy(tok_hbm.at[:, pl.ds(j * HD, HD)], kvx.at[j], lsem.at[j])

    def xw_load(i, slot):
        return pltpu.make_async_copy(w_xkv.at[pl.ds(i * 2 * XR, 2 * XR), :], xw.at[slot], xwsem.at[slot])

    def ctx_load(i, slot):
        return pltpu.make_async_copy(ctx_hbm.at[:, pl.ds(i * KEYS, KEYS)], cbuf.at[slot], csem.at[slot])

    wf_load = pltpu.make_async_copy(wf_hbm, wf, lsem.at[40])

    @pl.loop(0, 40)
    def _(j):
        tok_load(j).start()

    def kv_slot(kc):
        return (NT + HL * kc) % NSLOT

    def start_kv(kc):
        for m in range(2):
            for b in range(NB):
                start_heads(w_qkv.at[1 + m], kc, b, kv_slot(kc) + NB * m + b)

    barrier = pltpu.get_barrier_semaphore()
    for peer in (partner, across, diagonal, opposite):
        pl.semaphore_signal(barrier, inc=1, device_id=peer, device_id_type=MESH)

    scale = HD ** -0.5

    def attend(a, keys, values):
        rows = pl.ds(a * RH, RH)
        for h in range(HL):
            lanes = pl.ds(HD * (h % 2), HD)
            qh = qacc[h // 2, rows, lanes].astype(BF16)
            s1, s2 = [dot_nt(qh, k) * scale for k in keys(h)]
            m = jnp.max(jnp.maximum(s1, s2), axis=-1, keepdims=True)
            p1 = jnp.exp(s1 - m)
            p2 = jnp.exp(s2 - m)
            total = jnp.sum(p1 + p2, axis=-1, keepdims=True)
            v1, v2 = values(h)
            o = dot(p1.astype(BF16), v1) + dot(p2.astype(BF16), v2)
            obuf[h // 2, rows, lanes] = (o / total).astype(BF16)

    def d2d(a, i, g):
        src = part.at[pl.ds(i * g, g), pl.ds(pl.multiple_of(a * RH + (1 - c) * CB, OB), CB), :]
        return pltpu.make_async_remote_copy(src_ref=src, dst_ref=dsum.at[a, pl.ds(i * g, g)], send_sem=ds_s.at[a, i],
                                            recv_sem=ds_r.at[a, i], device_id=partner, device_id_type=MESH)

    def xsend(a, i, g):
        src = dsum.at[a, pl.ds(i * g, g), pl.ds(pl.multiple_of((1 - x) * OB, OB), OB), :]
        return pltpu.make_async_remote_copy(src_ref=src, dst_ref=xin.at[a, pl.ds(i * g, g)], send_sem=xs_s.at[a, i],
                                            recv_sem=xs_r.at[a, i], device_id=across, device_id_type=MESH)

    def core_sum(a, i, g):
        d2d(a, i, g).wait_recv()
        for u in range(g):
            t = i * g + u
            dsum[a, t] = dsum[a, t] + part[t, pl.ds(pl.multiple_of(a * RH + c * CB, OB), CB), :]

    def rs_loop(compute, compute_halves, send_halves, g, lag):
        iters = NT // g

        @pl.loop(0, iters + lag)
        def _(i):
            @pl.when(i < iters)
            def _():
                compute(i)

            @pl.when(i >= lag)
            def _():
                for a in send_halves:
                    core_sum(a, i - lag, g)

            @pl.when(i < iters)
            def _():
                for a in compute_halves:
                    d2d(a, i, g).start()

            @pl.when(i >= lag)
            def _():
                for a in send_halves:
                    xsend(a, i - lag, g).start()

    def hrows(core, chip, a):
        return pl.ds(pl.multiple_of(a * RH + core * CB + chip * OB, OB), OB)

    def gather_copy(buf, kc, rows, ssem, rsem_, peer):
        ref = buf.at[pl.ds(kc * NB, NB), rows, :]
        return pltpu.make_async_remote_copy(src_ref=ref, dst_ref=ref, send_sem=ssem, recv_sem=rsem_,
                                            device_id=peer, device_id_type=MESH)

    def g_across(a, kc, chip, buf=hbuf):
        return gather_copy(buf, kc, hrows(c, chip, a), ax_s.at[a, kc], ax_r.at[a, kc], across)

    def g_partner(a, kc, core, buf=hbuf):
        return gather_copy(buf, kc, hrows(core, x, a), ad_s.at[a, kc], ad_r.at[a, kc], partner)

    def g_forward(a, kc, core, buf=hbuf):
        return gather_copy(buf, kc, hrows(core, 1 - x, a), af_s.at[a, kc], af_r.at[a, kc], partner)

    def modrow(r, t, width=W):
        return mod_ref[r, 0:1, pl.ds(pl.multiple_of(t * width, width), width)]

    def residual(a, gate, drained):
        g = GA
        def body(i, acc):
            xsend(a, i, g).wait()
            if not drained:
                d2d(a, i, g).wait_send()
            for u in range(g):
                t = i * g + u
                proj = (dsum[a, t, pl.ds(pl.multiple_of(x * OB, OB), OB), :] + xin[a, t]).astype(BF16).astype(F32)
                if gate is not None:
                    proj = modrow(gate, t) * proj
                new = xres[a, t] + proj
                xres[a, t] = new
                acc = acc + new
            return acc
        acc = lax.fori_loop(0, NT // g, body, jnp.zeros((OB, W), F32))
        return jnp.sum(acc, axis=-1, keepdims=True)

    def stats(a, row_sum):
        mean = row_sum / D

        def body(i, acc):
            for u in range(KC):
                d_ = xres[a, i * KC + u] - mean
                acc = acc + d_ * d_
            return acc
        acc = lax.fori_loop(0, NT // KC, body, jnp.zeros((OB, W), F32))
        var = jnp.sum(acc, axis=-1, keepdims=True) / D
        return mean, lax.rsqrt(var + LN_EPS)

    def norm_and_send(a, gate, drained, shift, gain):
        mean, inv = stats(a, residual(a, gate, drained))

        @pl.loop(0, KC)
        def _(kc):
            for u in range(NB):
                t = kc * NB + u
                h = (xres[a, t] - mean) * inv
                if gain is not None:
                    h = h * (1.0 + modrow(gain, t)) + modrow(shift, t)
                hbuf[t, hrows(c, x, a), :] = h.astype(BF16)
            g_across(a, kc, x).start()
            g_partner(a, kc, c).start()

    def gather_forward(a, kc, buf=hbuf):
        g_across(a, kc, 1 - x, buf).wait_recv()
        g_forward(a, kc, c, buf).start()

    def gather_wait(a, kc, buf=hbuf):
        g_partner(a, kc, 1 - c, buf).wait_recv()
        g_forward(a, kc, 1 - c, buf).wait_recv()
        g_across(a, kc, x, buf).wait_send()
        g_partner(a, kc, c, buf).wait_send()
        g_forward(a, kc, c, buf).wait_send()

    def mm(lhs, slot):
        acc = dot(lhs(0), ring[slot, 0:W, :])
        for j in range(1, NB):
            acc = acc + dot(lhs(j), ring[slot, W * j:W * (j + 1), :])
        return acc

    def norm_tokens(blocks):
        spans = [pl.ds(pl.multiple_of(r0, OB), n) for r0, n, _ in blocks]
        zeros = tuple(jnp.zeros((n, HD), F32) for _, n, _ in blocks)

        def across_lanes(accs):
            return [jnp.sum(acc, axis=-1, keepdims=True) / D for acc in accs]

        def sums(i, accs):
            for u in range(4):
                accs = tuple(acc + kvx[i * 4 + u, r, :].astype(F32) for acc, r in zip(accs, spans))
            return accs
        means = across_lanes(lax.fori_loop(0, HL, sums, zeros))

        def squares(i, accs):
            for u in range(4):
                ds = [kvx[i * 4 + u, r, :].astype(F32) - mean for r, mean in zip(spans, means)]
                accs = tuple(acc + d_ * d_ for acc, d_ in zip(accs, ds))
            return accs
        invs = [lax.rsqrt(var + LN_EPS) for var in across_lanes(lax.fori_loop(0, HL, squares, zeros))]

        @pl.loop(0, NT)
        def _(t):
            for hh in range(2):
                gain = 1.0 + modrow(1, 2 * t + hh, HD)
                shift = modrow(0, 2 * t + hh, HD)
                lanes = pl.ds(HD * hh, HD)
                for (_, _, a), r, mean, inv in zip(blocks, spans, means, invs):
                    v = kvx[2 * t + hh, r, :].astype(F32)
                    if a is not None:
                        xres[a, t, :, lanes] = v
                    hbuf[t, r, lanes] = ((v - mean) * inv * gain + shift).astype(BF16)

    def y_copy(a, kc):
        rows = hrows(c, x, a)
        return pltpu.make_async_remote_copy(
            src_ref=hbuf.at[pl.ds(kc * NB, NB), rows, :], dst_ref=ubuf.at[pl.ds(kc * NB, NB), rows, :],
            send_sem=ys_s.at[a, kc], recv_sem=ys_r.at[a, kc], device_id=opposite, device_id_type=MESH)

    def y_forward(kc):
        for a in HALVES:
            y_copy(a, kc).wait_recv()
            g_across(a, kc, x, ubuf).start()
            g_partner(a, kc, c, ubuf).start()

    def kv_step(buf, kc, half):
        first = kv_slot(kc)
        base = HL * half

        if half == 0:
            for i in range(HL):
                wait_block(first + i)
        for i in range(HL):
            m, b = i // NB, i % NB
            acc = mm(lambda j: buf[kc * NB + j], first + i)
            if kc > 0:
                acc = part[base + i] + acc
            if kc < KC - 1:
                part[base + i] = acc
            else:
                kvs[m, 2 * b, W * half:W * (half + 1), :] = acc[:, 0:HD].astype(BF16)
                kvs[m, 2 * b + 1, W * half:W * (half + 1), :] = acc[:, HD:W].astype(BF16)

    with jax.named_scope("ln0"):
        @pl.loop(0, 40)
        def _(j):
            tok_load(j).wait()
        @pl.loop(0, NT)
        def _(i):
            start_heads(w_qkv.at[0], i // NB, i % NB, i)

        start_kv(0)
        start_kv(1)
        norm_tokens([(a * RH + c * CB + x * OB, OB, a) for a in HALVES])
        pl.semaphore_wait(barrier, KC)
        for kc in range(KC):
            for a in HALVES:
                y_copy(a, kc).start()
        norm_tokens([(a * RH + c * CB + (1 - x) * OB, OB, None) for a in HALVES]
                    + [(a * RH + (1 - c) * CB, CB, None) for a in HALVES])

    with jax.named_scope("q"):
        for kc in range(0, KC, 2):
            for i in range(2 * NB):
                wait_block(kc * NB + i)
            for b in range(NB):
                acc = mm(lambda j: hbuf[kc * NB + j], kc * NB + b)
                acc = acc + mm(lambda j: hbuf[(kc + 1) * NB + j], (kc + 1) * NB + b)
                qacc[b] = acc if kc == 0 else qacc[b] + acc
        start_kv(2)
        start_kv(3)

    def spread(kc):
        for a in HALVES:
            gather_forward(a, kc, ubuf)

    def other_kv(kc):
        for a in HALVES:
            gather_wait(a, kc, ubuf)
            y_copy(a, kc).wait_send()
        kv_step(ubuf, kc, 1)
        for i in range(HL):
            if kc < 2:
                start_cols(w_out, 0, HL * kc + i, kv_slot(kc) + i)
            else:
                j = HL * (kc - 2) + i
                start_heads(w_xq, j // NB, j % NB, kv_slot(kc) + i)

    with jax.named_scope("kv"):
        y_forward(0)
        kv_step(hbuf, 0, 0)
        kv_step(hbuf, 1, 0)
        y_forward(1)
        kv_step(hbuf, 2, 0)
        spread(0)
        y_forward(2)
        kv_step(hbuf, 3, 0)
        spread(1)
    with jax.named_scope("kvo"):
        other_kv(0)
        y_forward(3)
        other_kv(1)
        spread(2)
        other_kv(2)
        spread(3)
        other_kv(3)

    wf_load.start()
    for i in range(2):
        xw_load(i, i).start()
        ctx_load(i, i).start()

    for a in HALVES:
        rows = pl.ds(a * RH, RH)
        with jax.named_scope("attn1_%d" % a):
            attend(a, lambda h: [kvs[0, h, 0:W, :], kvs[0, h, W:2 * W, :]],
                   lambda h: [kvs[1, h, 0:W, :], kvs[1, h, W:2 * W, :]])

        def out_tiles(i):
            if a == 0:
                for u in range(GA):
                    wait_block(NT + i * GA + u)
            for u in range(GA):
                part[i * GA + u, rows, :] = mm(lambda j: obuf[j, rows, :], NT + i * GA + u)
            if a == HALVES[-1]:
                for u in range(GA):
                    start_cols(w_xout, 0, i * GA + u, NT + i * GA + u)

        with jax.named_scope("rs1_%d" % a):
            rs_loop(out_tiles, (a,), (a,), GA, 2)
    for a in HALVES:
        @pl.loop(0, NT // GA)
        def _(i):
            d2d(a, i, GA).wait_send()

    def text_kv():
        @pl.loop(0, XC)
        def _(i):
            for a in HALVES:
                @pl.when(i == 6 + 2 * a)
                def _():
                    norm_and_send(a, 2, True, None, None)

            slot = i % 2
            xw_load(i, slot).wait()
            for q in range(2):
                @pl.loop(0, XR // W)
                def _(r):
                    xf[q, pl.ds(pl.multiple_of(r * W, W), W), :] = (
                        xw[slot, pl.ds(pl.multiple_of(q * XR + r * W, W), W), :].astype(F32))

            @pl.when(i < XC - 2)
            def _():
                xw_load(i + 2, slot).start()
            ctx_load(i, slot).wait()

            for h in range(HL):
                top, low = part[2 * h], part[2 * h + 1]
                for q in range(2):
                    w = jnp.concatenate([xf[q, pl.ds(2 * h, W, stride=NT), :],
                                         xf[q, pl.ds(2 * h + 1, W, stride=NT), :]], axis=1).astype(BF16)
                    top = top + dot(cbuf[slot, 0:W, W * q:W * (q + 1)], w)
                    low = low + dot(cbuf[slot, W:2 * W, W * q:W * (q + 1)], w)
                part[2 * h] = top
                part[2 * h + 1] = low

            @pl.when(i < XC - 2)
            def _():
                ctx_load(i + 2, slot).start()

    with jax.named_scope("xkv"):
        @pl.loop(0, NT)
        def _(t):
            part[t] = jnp.zeros((W, W), F32)
        text_kv()

        @pl.loop(0, NT)
        def _(t):
            kvx[t] = part[t, :, 0:HD].astype(BF16)
            kvx[NT + t] = part[t, :, HD:W].astype(BF16)
    wf_load.wait()

    for a in HALVES:
        rows = pl.ds(a * RH, RH)
        last = a == HALVES[-1]
        for b in range(NB):
            qacc[b, rows, :] = jnp.zeros((RH, W), F32)

        gather_forward(a, 0)

        @pl.loop(0, KC)
        def _(kc):
            @pl.when(kc < KC - 1)
            def _():
                gather_forward(a, kc + 1)
            gather_wait(a, kc)
            if a == 0:
                for b in range(NB):
                    wait_block(kc * NB + b)
            for b in range(NB):
                qacc[b, rows, :] += mm(lambda j: hbuf[kc * NB + j, rows, :], kc * NB + b)
            if last:
                for b in range(NB):
                    start_cols(w_up, 0, kc * NB + b, kc * NB + b)

        with jax.named_scope("attn2_%d" % a):
            attend(a, lambda h: [kvx[2 * h], kvx[2 * h + 1]], lambda h: [kvx[NT + 2 * h], kvx[NT + 2 * h + 1]])

        def xout_tiles(i):
            if a == 0:
                for u in range(GA):
                    wait_block(NT + i * GA + u)
            for u in range(GA):
                part[i * GA + u, rows, :] = mm(lambda j: obuf[j, rows, :], NT + i * GA + u)
            if last:
                for u in range(GA):
                    start_cols(w_up, 1, i * GA + u, NT + i * GA + u)

        with jax.named_scope("rs2_%d" % a):
            rs_loop(xout_tiles, (a,), (a,), GA, 2)

    for a in HALVES:
        with jax.named_scope("fin2_%d" % a):
            norm_and_send(a, None, False, 3, KC)

    def up_step(kc, rows, refill):
        base = NT * (kc % 2)

        @pl.loop(0, NT // UP)
        def _(i):
            if rows != 1:
                for u in range(UP):
                    wait_block(base + i * UP + u)
            for u in range(UP):
                nb = i * UP + u
                r = pl.ds(0, ROWS) if rows is None else pl.ds(rows * RH, RH)
                acc = mm(lambda j: hbuf[kc * NB + j, r, :], base + nb)
                if kc > 0:
                    acc = part[nb, r, :] + acc
                if kc < KC - 1:
                    part[nb, r, :] = acc
                else:
                    ubuf[nb] = jax.nn.gelu(acc, approximate=True).astype(BF16)
            if refill:
                for u in range(UP):
                    nb = i * UP + u
                    if kc < 2:
                        start_cols(w_up, kc + 2, nb, base + nb)
                    else:
                        start_down(kc - 2, nb, base + nb)

    for a in HALVES:
        for kc in range(2):
            gather_forward(a, 2 * kc)
            gather_forward(a, 2 * kc + 1)
            gather_wait(a, kc)
            with jax.named_scope("up%d_%d" % (kc, a)):
                up_step(kc, a, a == HALVES[-1])
    for kc in range(2, KC):
        for a in HALVES:
            gather_wait(a, kc)
        with jax.named_scope("up%d" % kc):
            up_step(kc, None, True)

    def xsend_both(t):
        src = dsum.at[:, t, pl.ds(pl.multiple_of((1 - x) * OB, OB), OB), :]
        return pltpu.make_async_remote_copy(src_ref=src, dst_ref=xin.at[:, t], send_sem=xs_s.at[0, t],
                                            recv_sem=xs_r.at[0, t], device_id=across, device_id_type=MESH)

    def down_slot(t, kc):
        return NT * (t // NB % 2) + KC * (t % NB) + kc

    with jax.named_scope("down"):
        @pl.loop(0, NT + 1)
        def _(t):
            @pl.when(t < NT)
            def _():
                for kc in range(KC):
                    wait_block(down_slot(t, kc))
                acc = mm(lambda j: ubuf[j], down_slot(t, 0))
                for kc in range(1, KC):
                    acc = acc + mm(lambda j: ubuf[NB * kc + j], down_slot(t, kc))
                part[t] = acc

            @pl.when(t < HL)
            def _():
                for kc in range(KC):
                    start_cols(w_down, kc, t + HL, down_slot(t, kc))

            @pl.when(t > 0)
            def _():
                for a in HALVES:
                    core_sum(a, t - 1, 1)

            @pl.when(t < NT)
            def _():
                for a in HALVES:
                    d2d(a, t, 1).start()

            @pl.when(t > 0)
            def _():
                xsend_both(t - 1).start()

    def out_copy(a, peer, k, core, chip):
        ref = obout.at[hrows(core, chip, a), :]
        return pltpu.make_async_remote_copy(src_ref=ref, dst_ref=ref, send_sem=os_s.at[a, k], recv_sem=os_r.at[a, k],
                                            device_id=peer, device_id_type=MESH)

    with jax.named_scope("last_sum"):
        def last_residual(t, accs):
            xsend_both(t).wait()
            news = []
            for a in HALVES:
                d2d(a, t, 1).wait_send()
                proj = dsum[a, t, pl.ds(pl.multiple_of(x * OB, OB), OB), :] + xin[a, t]
                new = xres[a, t] + modrow(NB, t) * proj.astype(BF16).astype(F32)
                xres[a, t] = new
                news.append(new)
            return tuple(acc + new for acc, new in zip(accs, news))
        zeros = tuple(jnp.zeros((OB, W), F32) for a in HALVES)
        sums = lax.fori_loop(0, NT, last_residual, zeros)
    with jax.named_scope("last_norm"):
        means = [jnp.sum(acc, axis=-1, keepdims=True) / D for acc in sums]

        def squares(i, accs):
            for u in range(4):
                ds = [xres[a, i * 4 + u] - means[a] for a in HALVES]
                accs = tuple(acc + d_ * d_ for acc, d_ in zip(accs, ds))
            return accs
        invs = [lax.rsqrt(jnp.sum(acc, axis=-1, keepdims=True) / D + LN_EPS)
                for acc in lax.fori_loop(0, NT // 4, squares, zeros)]

        def project(i, acc):
            for u in range(4):
                t = i * 4 + u
                fin = jnp.concatenate([(xres[a, t] - means[a]) * invs[a] for a in HALVES], axis=0).astype(BF16)
                acc = acc + dot_nt(fin, wf[:, pl.ds(pl.multiple_of(t * W, W), W)])
            return acc
        acc = lax.fori_loop(0, NT // 4, project, jnp.zeros((NH * OB, 64), F32))
        acc = jnp.concatenate([acc, jnp.zeros((NH * OB, 64), F32)], axis=1)
        for a in HALVES:
            obout[hrows(c, x, a), :] = acc[a * OB:(a + 1) * OB, :]
            out_copy(a, across, 0, c, x).start()
            out_copy(a, partner, 1, c, x).start()
            out_copy(a, diagonal, 2, c, x).start()
    for a in HALVES:
        out_copy(a, across, 0, c, 1 - x).wait()
        out_copy(a, partner, 1, 1 - c, x).wait()
        out_copy(a, diagonal, 2, 1 - c, 1 - x).wait()
    out_ref[...] = jnp.transpose(obout[...])[0:64, :]


def block_call(args):
    any_spec = pl.BlockSpec(memory_space=pl.ANY)
    vmem_spec = pl.BlockSpec(memory_space=pltpu.VMEM)
    sem = pltpu.SemaphoreType.DMA
    return pl.pallas_call(
        block_kernel,
        out_shape=jax.ShapeDtypeStruct((64, ROWS), F32),
        in_specs=[any_spec] * 2 + [vmem_spec] + [any_spec] * 8,
        out_specs=vmem_spec,
        scratch_shapes=[
            pltpu.VMEM((NSLOT, KD, W), BF16),
            pltpu.VMEM((NT, ROWS, W), F32),
            pltpu.VMEM((NH, NT, CB, W), F32),
            pltpu.VMEM((NH, NT, OB, W), F32),
            pltpu.VMEM((NH, NT, OB, W), F32),
            pltpu.VMEM((NT, ROWS, W), BF16),
            pltpu.VMEM((NT, ROWS, W), BF16),
            pltpu.VMEM((NB, ROWS, W), F32),
            pltpu.VMEM((NB, ROWS, W), BF16),
            pltpu.VMEM((2, HL, KEYS, HD), BF16),
            pltpu.VMEM((2 * NT, W, HD), BF16),
            pltpu.VMEM((2, 2 * XR, HD), BF16),
            pltpu.VMEM((2, XR, HD), F32),
            pltpu.VMEM((2, KEYS, KEYS), BF16),
            pltpu.VMEM((64, D), BF16),
            pltpu.VMEM((ROWS, HD), F32),
            sem((NSLOT,)), sem((41,)), sem((2,)), sem((2,)),
            sem((NH, NT)), sem((NH, NT)), sem((NH, NT)), sem((NH, NT)),
            sem((NH, KC)), sem((NH, KC)), sem((NH, KC)), sem((NH, KC)), sem((NH, KC)), sem((NH, KC)),
            sem((NH, KC)), sem((NH, KC)),
            sem((NH, 3)), sem((NH, 3)),
        ],
        compiler_params=pltpu.CompilerParams(collective_id=0, has_side_effects=True, vmem_limit_bytes=67_000_000),
        cost_estimate=pl.CostEstimate(flops=60 * 10**9, bytes_accessed=218 * 10**6, transcendentals=4 * 10**6),
        name='dit_block',
    )(*args)


def solution(mesh):
    def device_step(tokens, context, modulation, w_qkv, w_out, w_xq, w_xkv, w_xout, w_up, w_down, w_final):
        return jnp.transpose(block_call((
            tokens, context, jnp.transpose(modulation, (1, 0, 2)),
            jnp.transpose(w_qkv[0], (1, 2, 0, 3)), jnp.transpose(w_xkv[0], (0, 2, 1, 3)).reshape(2 * HL * D, HD),
            w_out[0].reshape(KD, D), jnp.transpose(w_xq[0], (1, 0, 2)), w_xout[0].reshape(KD, D),
            w_up[0], w_down[0], jnp.transpose(w_final))))

    in_specs = (P('sp', None), P(), P(), P(None, None, None, 'tp', None), P(None, 'tp', None, None),
                P(None, None, 'tp', None), P(None, None, None, 'tp', None), P(None, 'tp', None, None),
                P(None, None, 'tp'), P(None, 'tp', None), P())
    return jax.shard_map(device_step, mesh=mesh, in_specs=in_specs, out_specs=P('sp', None), check_vma=False)
```

```python
import functools
import jax
import jax.numpy as jnp
from jax import lax
from jax.experimental import pallas as pl
from jax.experimental.pallas import tpu as pltpu
from jax.sharding import PartitionSpec as P

F32 = jnp.float32
BF16 = jnp.bfloat16
LN_EPS = 1e-6
MESH = pl.DeviceIdType.MESH

W = 256
HD = 128
KD = 1280
NB = 5
KEYS = 512
D = 5120
ROWS = 256
NT = 20
KC = 4
HL = 10
NH = 2
RH = ROWS // NH
CB = RH // 2
OB = RH // 4
NSLOT = 40
HALVES = tuple(range(NH))
UP = 10
GA = 4
XC = 10
XR = 256 * 2 * HL


def dot(a, b):
    return jnp.dot(a, b, preferred_element_type=F32)


def dot_nt(a, b):
    return lax.dot_general(a, b, (((1,), (1,)), ((), ())), preferred_element_type=F32)


def block_kernel(tok_hbm, ctx_hbm, mod_ref, w_qkv, w_xkv, w_out, w_xq, w_xout, w_up, w_down, wf_hbm,
                 out_ref,
                 ring, part, dsum, xin, xres, hbuf, ubuf, qacc, obuf, kvs, kvx, xw, xf, cbuf, wf, obout,
                 rsem, lsem, xwsem, csem, ds_s, ds_r, xs_s, xs_r, ax_s, ax_r, ad_s, ad_r, af_s, af_r, ys_s, ys_r,
                 os_s, os_r):
    sp = lax.axis_index('sp')
    tp = lax.axis_index('tp')
    x = tp // 2
    c = tp % 2
    partner = (sp, 2 * x + (1 - c))
    across = (sp, 2 * (1 - x) + c)
    diagonal = (sp, 2 * (1 - x) + (1 - c))
    opposite = (1 - sp, tp)

    def kslice(kc):
        return pl.ds(kc * KD, KD)

    def nslice(nb):
        return pl.ds(nb * W, W)

    def start_cols(w, kc, nb, slot):
        pltpu.make_async_copy(w.at[kslice(kc), nslice(nb)], ring.at[slot], rsem.at[slot]).start()

    def start_heads(w, kc, b, slot):
        for hh in range(2):
            pltpu.make_async_copy(w.at[2 * b + hh, kslice(kc), :], ring.at[slot, :, pl.ds(HD * hh, HD)],
                                  rsem.at[slot]).start()

    def wait_block(slot):
        pltpu.make_async_copy(w_out.at[pl.ds(0, KD), pl.ds(0, W)], ring.at[slot], rsem.at[slot]).wait()

    def start_down(g, i, slot):
        start_cols(w_down, i % KC, NB * g + i // KC, slot)

    def tok_load(j):
        return pltpu.make_async_copy(tok_hbm.at[:, pl.ds(j * HD, HD)], kvx.at[j], lsem.at[j])

    def xw_load(i, slot):
        return pltpu.make_async_copy(w_xkv.at[pl.ds(i * 2 * XR, 2 * XR), :], xw.at[slot], xwsem.at[slot])

    def ctx_load(i, slot):
        return pltpu.make_async_copy(ctx_hbm.at[:, pl.ds(i * KEYS, KEYS)], cbuf.at[slot], csem.at[slot])

    wf_load = pltpu.make_async_copy(wf_hbm, wf, lsem.at[40])

    @pl.loop(0, 40)
    def _(j):
        tok_load(j).start()

    def kv_slot(kc):
        return (NT + HL * kc) % NSLOT

    def start_kv(kc):
        for m in range(2):
            for b in range(NB):
                start_heads(w_qkv.at[1 + m], kc, b, kv_slot(kc) + NB * m + b)

    barrier = pltpu.get_barrier_semaphore()
    for peer in (partner, across, diagonal, opposite):
        pl.semaphore_signal(barrier, inc=1, device_id=peer, device_id_type=MESH)

    scale = HD ** -0.5

    def attend(a, keys, values):
        rows = pl.ds(a * RH, RH)
        for h in range(HL):
            lanes = pl.ds(HD * (h % 2), HD)
            qh = qacc[h // 2, rows, lanes].astype(BF16)
            s1, s2 = [dot_nt(qh, k) * scale for k in keys(h)]
            m = jnp.max(jnp.maximum(s1, s2), axis=-1, keepdims=True)
            p1 = jnp.exp(s1 - m)
            p2 = jnp.exp(s2 - m)
            total = jnp.sum(p1 + p2, axis=-1, keepdims=True)
            v1, v2 = values(h)
            o = dot(p1.astype(BF16), v1) + dot(p2.astype(BF16), v2)
            obuf[h // 2, rows, lanes] = (o / total).astype(BF16)

    def d2d(a, i, g):
        src = part.at[pl.ds(i * g, g), pl.ds(pl.multiple_of(a * RH + (1 - c) * CB, OB), CB), :]
        return pltpu.make_async_remote_copy(src_ref=src, dst_ref=dsum.at[a, pl.ds(i * g, g)], send_sem=ds_s.at[a, i],
                                            recv_sem=ds_r.at[a, i], device_id=partner, device_id_type=MESH)

    def xsend(a, i, g):
        src = dsum.at[a, pl.ds(i * g, g), pl.ds(pl.multiple_of((1 - x) * OB, OB), OB), :]
        return pltpu.make_async_remote_copy(src_ref=src, dst_ref=xin.at[a, pl.ds(i * g, g)], send_sem=xs_s.at[a, i],
                                            recv_sem=xs_r.at[a, i], device_id=across, device_id_type=MESH)

    def core_sum(a, i, g):
        d2d(a, i, g).wait_recv()
        for u in range(g):
            t = i * g + u
            dsum[a, t] = dsum[a, t] + part[t, pl.ds(pl.multiple_of(a * RH + c * CB, OB), CB), :]

    def rs_loop(compute, compute_halves, send_halves, g, lag):
        iters = NT // g

        @pl.loop(0, iters + lag)
        def _(i):
            @pl.when(i < iters)
            def _():
                compute(i)

            @pl.when(i >= lag)
            def _():
                for a in send_halves:
                    core_sum(a, i - lag, g)

            @pl.when(i < iters)
            def _():
                for a in compute_halves:
                    d2d(a, i, g).start()

            @pl.when(i >= lag)
            def _():
                for a in send_halves:
                    xsend(a, i - lag, g).start()

    def hrows(core, chip, a):
        return pl.ds(pl.multiple_of(a * RH + core * CB + chip * OB, OB), OB)

    def gather_copy(buf, kc, rows, ssem, rsem_, peer):
        ref = buf.at[pl.ds(kc * NB, NB), rows, :]
        return pltpu.make_async_remote_copy(src_ref=ref, dst_ref=ref, send_sem=ssem, recv_sem=rsem_,
                                            device_id=peer, device_id_type=MESH)

    def g_across(a, kc, chip, buf=hbuf):
        return gather_copy(buf, kc, hrows(c, chip, a), ax_s.at[a, kc], ax_r.at[a, kc], across)

    def g_partner(a, kc, core, buf=hbuf):
        return gather_copy(buf, kc, hrows(core, x, a), ad_s.at[a, kc], ad_r.at[a, kc], partner)

    def g_forward(a, kc, core, buf=hbuf):
        return gather_copy(buf, kc, hrows(core, 1 - x, a), af_s.at[a, kc], af_r.at[a, kc], partner)

    def modrow(r, t, width=W):
        return mod_ref[r, 0:1, pl.ds(pl.multiple_of(t * width, width), width)]

    def residual(a, gate, drained):
        g = GA
        def body(i, acc):
            xsend(a, i, g).wait()
            if not drained:
                d2d(a, i, g).wait_send()
            for u in range(g):
                t = i * g + u
                proj = (dsum[a, t, pl.ds(pl.multiple_of(x * OB, OB), OB), :] + xin[a, t]).astype(BF16).astype(F32)
                if gate is not None:
                    proj = modrow(gate, t) * proj
                new = xres[a, t] + proj
                xres[a, t] = new
                acc = acc + new
            return acc
        acc = lax.fori_loop(0, NT // g, body, jnp.zeros((OB, W), F32))
        return jnp.sum(acc, axis=-1, keepdims=True)

    def stats(a, row_sum):
        mean = row_sum / D

        def body(i, acc):
            for u in range(KC):
                d_ = xres[a, i * KC + u] - mean
                acc = acc + d_ * d_
            return acc
        acc = lax.fori_loop(0, NT // KC, body, jnp.zeros((OB, W), F32))
        var = jnp.sum(acc, axis=-1, keepdims=True) / D
        return mean, lax.rsqrt(var + LN_EPS)

    def norm_and_send(a, gate, drained, shift, gain):
        mean, inv = stats(a, residual(a, gate, drained))

        @pl.loop(0, KC)
        def _(kc):
            for u in range(NB):
                t = kc * NB + u
                h = (xres[a, t] - mean) * inv
                if gain is not None:
                    h = h * (1.0 + modrow(gain, t)) + modrow(shift, t)
                hbuf[t, hrows(c, x, a), :] = h.astype(BF16)
            g_across(a, kc, x).start()
            g_partner(a, kc, c).start()

    def gather_forward(a, kc, buf=hbuf):
        g_across(a, kc, 1 - x, buf).wait_recv()
        g_forward(a, kc, c, buf).start()

    def gather_wait(a, kc, buf=hbuf):
        g_partner(a, kc, 1 - c, buf).wait_recv()
        g_forward(a, kc, 1 - c, buf).wait_recv()
        g_across(a, kc, x, buf).wait_send()
        g_partner(a, kc, c, buf).wait_send()
        g_forward(a, kc, c, buf).wait_send()

    def mm(lhs, slot):
        acc = dot(lhs(0), ring[slot, 0:W, :])
        for j in range(1, NB):
            acc = acc + dot(lhs(j), ring[slot, W * j:W * (j + 1), :])
        return acc

    def norm_tokens(blocks):
        spans = [pl.ds(pl.multiple_of(r0, OB), n) for r0, n, _ in blocks]
        zeros = tuple(jnp.zeros((n, HD), F32) for _, n, _ in blocks)

        def across_lanes(accs):
            return [jnp.sum(acc, axis=-1, keepdims=True) / D for acc in accs]

        def sums(i, accs):
            for u in range(4):
                accs = tuple(acc + kvx[i * 4 + u, r, :].astype(F32) for acc, r in zip(accs, spans))
            return accs
        means = across_lanes(lax.fori_loop(0, HL, sums, zeros))

        def squares(i, accs):
            for u in range(4):
                ds = [kvx[i * 4 + u, r, :].astype(F32) - mean for r, mean in zip(spans, means)]
                accs = tuple(acc + d_ * d_ for acc, d_ in zip(accs, ds))
            return accs
        invs = [lax.rsqrt(var + LN_EPS) for var in across_lanes(lax.fori_loop(0, HL, squares, zeros))]

        @pl.loop(0, NT)
        def _(t):
            for hh in range(2):
                gain = 1.0 + modrow(1, 2 * t + hh, HD)
                shift = modrow(0, 2 * t + hh, HD)
                lanes = pl.ds(HD * hh, HD)
                for (_, _, a), r, mean, inv in zip(blocks, spans, means, invs):
                    v = kvx[2 * t + hh, r, :].astype(F32)
                    if a is not None:
                        xres[a, t, :, lanes] = v
                    hbuf[t, r, lanes] = ((v - mean) * inv * gain + shift).astype(BF16)

    def y_copy(a, kc):
        rows = hrows(c, x, a)
        return pltpu.make_async_remote_copy(
            src_ref=hbuf.at[pl.ds(kc * NB, NB), rows, :], dst_ref=ubuf.at[pl.ds(kc * NB, NB), rows, :],
            send_sem=ys_s.at[a, kc], recv_sem=ys_r.at[a, kc], device_id=opposite, device_id_type=MESH)

    def y_forward(kc):
        for a in HALVES:
            y_copy(a, kc).wait_recv()
            g_across(a, kc, x, ubuf).start()
            g_partner(a, kc, c, ubuf).start()

    def kv_step(buf, kc, half):
        first = kv_slot(kc)
        base = HL * half

        if half == 0:
            for i in range(HL):
                wait_block(first + i)
        for i in range(HL):
            m, b = i // NB, i % NB
            acc = mm(lambda j: buf[kc * NB + j], first + i)
            if kc > 0:
                acc = part[base + i] + acc
            if kc < KC - 1:
                part[base + i] = acc
            else:
                kvs[m, 2 * b, W * half:W * (half + 1), :] = acc[:, 0:HD].astype(BF16)
                kvs[m, 2 * b + 1, W * half:W * (half + 1), :] = acc[:, HD:W].astype(BF16)

    with jax.named_scope("ln0"):
        @pl.loop(0, 40)
        def _(j):
            tok_load(j).wait()
        @pl.loop(0, NT)
        def _(i):
            start_heads(w_qkv.at[0], i // NB, i % NB, i)

        start_kv(0)
        start_kv(1)
        norm_tokens([(a * RH + c * CB + x * OB, OB, a) for a in HALVES])
        pl.semaphore_wait(barrier, KC)
        for kc in range(KC):
            for a in HALVES:
                y_copy(a, kc).start()
        norm_tokens([(a * RH + c * CB + (1 - x) * OB, OB, None) for a in HALVES]
                    + [(a * RH + (1 - c) * CB, CB, None) for a in HALVES])

    with jax.named_scope("q"):
        for kc in range(0, KC, 2):
            for i in range(2 * NB):
                wait_block(kc * NB + i)
            for b in range(NB):
                acc = mm(lambda j: hbuf[kc * NB + j], kc * NB + b)
                acc = acc + mm(lambda j: hbuf[(kc + 1) * NB + j], (kc + 1) * NB + b)
                qacc[b] = acc if kc == 0 else qacc[b] + acc
        start_kv(2)
        start_kv(3)

    def spread(kc):
        for a in HALVES:
            gather_forward(a, kc, ubuf)

    def other_kv(kc):
        for a in HALVES:
            gather_wait(a, kc, ubuf)
            y_copy(a, kc).wait_send()
        kv_step(ubuf, kc, 1)
        for i in range(HL):
            if kc < 2:
                start_cols(w_out, 0, HL * kc + i, kv_slot(kc) + i)
            else:
                j = HL * (kc - 2) + i
                start_heads(w_xq, j // NB, j % NB, kv_slot(kc) + i)

    with jax.named_scope("kv"):
        y_forward(0)
        kv_step(hbuf, 0, 0)
        kv_step(hbuf, 1, 0)
        y_forward(1)
        kv_step(hbuf, 2, 0)
        spread(0)
        y_forward(2)
        kv_step(hbuf, 3, 0)
        spread(1)
    with jax.named_scope("kvo"):
        other_kv(0)
        y_forward(3)
        other_kv(1)
        spread(2)
        other_kv(2)
        spread(3)
        other_kv(3)

    wf_load.start()
    for i in range(2):
        xw_load(i, i).start()
        ctx_load(i, i).start()

    for a in HALVES:
        rows = pl.ds(a * RH, RH)
        with jax.named_scope("attn1_%d" % a):
            attend(a, lambda h: [kvs[0, h, 0:W, :], kvs[0, h, W:2 * W, :]],
                   lambda h: [kvs[1, h, 0:W, :], kvs[1, h, W:2 * W, :]])

        def out_tiles(i):
            if a == 0:
                for u in range(GA):
                    wait_block(NT + i * GA + u)
            for u in range(GA):
                part[i * GA + u, rows, :] = mm(lambda j: obuf[j, rows, :], NT + i * GA + u)
            if a == HALVES[-1]:
                for u in range(GA):
                    start_cols(w_xout, 0, i * GA + u, NT + i * GA + u)

        with jax.named_scope("rs1_%d" % a):
            rs_loop(out_tiles, (a,), (a,), GA, 2)
    for a in HALVES:
        @pl.loop(0, NT // GA)
        def _(i):
            d2d(a, i, GA).wait_send()

    def text_kv():
        @pl.loop(0, XC)
        def _(i):
            for a in HALVES:
                @pl.when(i == 7 + 2 * a)
                def _():
                    norm_and_send(a, 2, True, None, None)

            slot = i % 2
            xw_load(i, slot).wait()
            for q in range(2):
                @pl.loop(0, XR // W)
                def _(r):
                    xf[q, pl.ds(pl.multiple_of(r * W, W), W), :] = (
                        xw[slot, pl.ds(pl.multiple_of(q * XR + r * W, W), W), :].astype(F32))

            @pl.when(i < XC - 2)
            def _():
                xw_load(i + 2, slot).start()
            ctx_load(i, slot).wait()

            for h in range(HL):
                top, low = part[2 * h], part[2 * h + 1]
                for q in range(2):
                    w = jnp.concatenate([xf[q, pl.ds(2 * h, W, stride=NT), :],
                                         xf[q, pl.ds(2 * h + 1, W, stride=NT), :]], axis=1).astype(BF16)
                    top = top + dot(cbuf[slot, 0:W, W * q:W * (q + 1)], w)
                    low = low + dot(cbuf[slot, W:2 * W, W * q:W * (q + 1)], w)
                part[2 * h] = top
                part[2 * h + 1] = low

            @pl.when(i < XC - 2)
            def _():
                ctx_load(i + 2, slot).start()

    with jax.named_scope("xkv"):
        @pl.loop(0, NT)
        def _(t):
            part[t] = jnp.zeros((W, W), F32)
        text_kv()

        @pl.loop(0, NT)
        def _(t):
            kvx[t] = part[t, :, 0:HD].astype(BF16)
            kvx[NT + t] = part[t, :, HD:W].astype(BF16)
    wf_load.wait()

    for a in HALVES:
        rows = pl.ds(a * RH, RH)
        last = a == HALVES[-1]
        for b in range(NB):
            qacc[b, rows, :] = jnp.zeros((RH, W), F32)

        gather_forward(a, 0)

        @pl.loop(0, KC)
        def _(kc):
            @pl.when(kc < KC - 1)
            def _():
                gather_forward(a, kc + 1)
            gather_wait(a, kc)
            if a == 0:
                for b in range(NB):
                    wait_block(kc * NB + b)
            for b in range(NB):
                qacc[b, rows, :] += mm(lambda j: hbuf[kc * NB + j, rows, :], kc * NB + b)
            if last:
                for b in range(NB):
                    start_cols(w_up, 0, kc * NB + b, kc * NB + b)

        with jax.named_scope("attn2_%d" % a):
            attend(a, lambda h: [kvx[2 * h], kvx[2 * h + 1]], lambda h: [kvx[NT + 2 * h], kvx[NT + 2 * h + 1]])

        def xout_tiles(i):
            if a == 0:
                for u in range(GA):
                    wait_block(NT + i * GA + u)
            for u in range(GA):
                part[i * GA + u, rows, :] = mm(lambda j: obuf[j, rows, :], NT + i * GA + u)
            if last:
                for u in range(GA):
                    start_cols(w_up, 1, i * GA + u, NT + i * GA + u)

        with jax.named_scope("rs2_%d" % a):
            rs_loop(xout_tiles, (a,), (a,), GA, 2)

    for a in HALVES:
        with jax.named_scope("fin2_%d" % a):
            norm_and_send(a, None, False, 3, KC)

    def up_step(kc, rows, refill):
        base = NT * (kc % 2)

        @pl.loop(0, NT // UP)
        def _(i):
            if rows != 1:
                for u in range(UP):
                    wait_block(base + i * UP + u)
            for u in range(UP):
                nb = i * UP + u
                r = pl.ds(0, ROWS) if rows is None else pl.ds(rows * RH, RH)
                acc = mm(lambda j: hbuf[kc * NB + j, r, :], base + nb)
                if kc > 0:
                    acc = part[nb, r, :] + acc
                if kc < KC - 1:
                    part[nb, r, :] = acc
                else:
                    ubuf[nb] = jax.nn.gelu(acc, approximate=True).astype(BF16)
            if refill:
                for u in range(UP):
                    nb = i * UP + u
                    if kc < 2:
                        start_cols(w_up, kc + 2, nb, base + nb)
                    else:
                        start_down(kc - 2, nb, base + nb)

    for a in HALVES:
        for kc in range(2):
            gather_forward(a, 2 * kc)
            gather_forward(a, 2 * kc + 1)
            gather_wait(a, kc)
            with jax.named_scope("up%d_%d" % (kc, a)):
                up_step(kc, a, a == HALVES[-1])
    for kc in range(2, KC):
        for a in HALVES:
            gather_wait(a, kc)
        with jax.named_scope("up%d" % kc):
            up_step(kc, None, True)

    def xsend_both(t):
        src = dsum.at[:, t, pl.ds(pl.multiple_of((1 - x) * OB, OB), OB), :]
        return pltpu.make_async_remote_copy(src_ref=src, dst_ref=xin.at[:, t], send_sem=xs_s.at[0, t],
                                            recv_sem=xs_r.at[0, t], device_id=across, device_id_type=MESH)

    def down_slot(t, kc):
        return NT * (t // NB % 2) + KC * (t % NB) + kc

    with jax.named_scope("down"):
        @pl.loop(0, NT + 1)
        def _(t):
            @pl.when(t < NT)
            def _():
                for kc in range(KC):
                    wait_block(down_slot(t, kc))
                acc = mm(lambda j: ubuf[j], down_slot(t, 0))
                for kc in range(1, KC):
                    acc = acc + mm(lambda j: ubuf[NB * kc + j], down_slot(t, kc))
                part[t] = acc

            @pl.when(t < HL)
            def _():
                for kc in range(KC):
                    start_cols(w_down, kc, t + HL, down_slot(t, kc))

            @pl.when(t > 0)
            def _():
                for a in HALVES:
                    core_sum(a, t - 1, 1)

            @pl.when(t < NT)
            def _():
                for a in HALVES:
                    d2d(a, t, 1).start()

            @pl.when(t > 0)
            def _():
                xsend_both(t - 1).start()

    def out_copy(a, peer, k, core, chip):
        ref = obout.at[hrows(core, chip, a), :]
        return pltpu.make_async_remote_copy(src_ref=ref, dst_ref=ref, send_sem=os_s.at[a, k], recv_sem=os_r.at[a, k],
                                            device_id=peer, device_id_type=MESH)

    with jax.named_scope("last_sum"):
        def last_residual(t, accs):
            xsend_both(t).wait()
            news = []
            for a in HALVES:
                d2d(a, t, 1).wait_send()
                proj = dsum[a, t, pl.ds(pl.multiple_of(x * OB, OB), OB), :] + xin[a, t]
                new = xres[a, t] + modrow(NB, t) * proj.astype(BF16).astype(F32)
                xres[a, t] = new
                news.append(new)
            return tuple(acc + new for acc, new in zip(accs, news))
        zeros = tuple(jnp.zeros((OB, W), F32) for a in HALVES)
        sums = lax.fori_loop(0, NT, last_residual, zeros)
    with jax.named_scope("last_norm"):
        means = [jnp.sum(acc, axis=-1, keepdims=True) / D for acc in sums]

        def squares(i, accs):
            for u in range(4):
                ds = [xres[a, i * 4 + u] - means[a] for a in HALVES]
                accs = tuple(acc + d_ * d_ for acc, d_ in zip(accs, ds))
            return accs
        invs = [lax.rsqrt(jnp.sum(acc, axis=-1, keepdims=True) / D + LN_EPS)
                for acc in lax.fori_loop(0, NT // 4, squares, zeros)]

        def project(i, acc):
            for u in range(4):
                t = i * 4 + u
                fin = jnp.concatenate([(xres[a, t] - means[a]) * invs[a] for a in HALVES], axis=0).astype(BF16)
                acc = acc + dot_nt(fin, wf[:, pl.ds(pl.multiple_of(t * W, W), W)])
            return acc
        acc = lax.fori_loop(0, NT // 4, project, jnp.zeros((NH * OB, 64), F32))
        acc = jnp.concatenate([acc, jnp.zeros((NH * OB, 64), F32)], axis=1)
        for a in HALVES:
            obout[hrows(c, x, a), :] = acc[a * OB:(a + 1) * OB, :]
            out_copy(a, across, 0, c, x).start()
            out_copy(a, partner, 1, c, x).start()
            out_copy(a, diagonal, 2, c, x).start()
    for a in HALVES:
        out_copy(a, across, 0, c, 1 - x).wait()
        out_copy(a, partner, 1, 1 - c, x).wait()
        out_copy(a, diagonal, 2, 1 - c, 1 - x).wait()
    out_ref[...] = jnp.transpose(obout[...])[0:64, :]


def block_call(args):
    any_spec = pl.BlockSpec(memory_space=pl.ANY)
    vmem_spec = pl.BlockSpec(memory_space=pltpu.VMEM)
    sem = pltpu.SemaphoreType.DMA
    return pl.pallas_call(
        block_kernel,
        out_shape=jax.ShapeDtypeStruct((64, ROWS), F32),
        in_specs=[any_spec] * 2 + [vmem_spec] + [any_spec] * 8,
        out_specs=vmem_spec,
        scratch_shapes=[
            pltpu.VMEM((NSLOT, KD, W), BF16),
            pltpu.VMEM((NT, ROWS, W), F32),
            pltpu.VMEM((NH, NT, CB, W), F32),
            pltpu.VMEM((NH, NT, OB, W), F32),
            pltpu.VMEM((NH, NT, OB, W), F32),
            pltpu.VMEM((NT, ROWS, W), BF16),
            pltpu.VMEM((NT, ROWS, W), BF16),
            pltpu.VMEM((NB, ROWS, W), F32),
            pltpu.VMEM((NB, ROWS, W), BF16),
            pltpu.VMEM((2, HL, KEYS, HD), BF16),
            pltpu.VMEM((2 * NT, W, HD), BF16),
            pltpu.VMEM((2, 2 * XR, HD), BF16),
            pltpu.VMEM((2, XR, HD), F32),
            pltpu.VMEM((2, KEYS, KEYS), BF16),
            pltpu.VMEM((64, D), BF16),
            pltpu.VMEM((ROWS, HD), F32),
            sem((NSLOT,)), sem((41,)), sem((2,)), sem((2,)),
            sem((NH, NT)), sem((NH, NT)), sem((NH, NT)), sem((NH, NT)),
            sem((NH, KC)), sem((NH, KC)), sem((NH, KC)), sem((NH, KC)), sem((NH, KC)), sem((NH, KC)),
            sem((NH, KC)), sem((NH, KC)),
            sem((NH, 3)), sem((NH, 3)),
        ],
        compiler_params=pltpu.CompilerParams(collective_id=0, has_side_effects=True, vmem_limit_bytes=67_000_000),
        cost_estimate=pl.CostEstimate(flops=60 * 10**9, bytes_accessed=218 * 10**6, transcendentals=4 * 10**6),
        name='dit_block',
    )(*args)


def solution(mesh):
    def device_step(tokens, context, modulation, w_qkv, w_out, w_xq, w_xkv, w_xout, w_up, w_down, w_final):
        return jnp.transpose(block_call((
            tokens, context, jnp.transpose(modulation, (1, 0, 2)),
            jnp.transpose(w_qkv[0], (1, 2, 0, 3)), jnp.transpose(w_xkv[0], (0, 2, 1, 3)).reshape(2 * HL * D, HD),
            w_out[0].reshape(KD, D), jnp.transpose(w_xq[0], (1, 0, 2)), w_xout[0].reshape(KD, D),
            w_up[0], w_down[0], jnp.transpose(w_final))))

    in_specs = (P('sp', None), P(), P(), P(None, None, None, 'tp', None), P(None, 'tp', None, None),
                P(None, None, 'tp', None), P(None, None, None, 'tp', None), P(None, 'tp', None, None),
                P(None, None, 'tp'), P(None, 'tp', None), P())
    return jax.shard_map(device_step, mesh=mesh, in_specs=in_specs, out_specs=P('sp', None), check_vma=False)
```
